128 devices in a mesh: row: 8 (over x, core), col: 16 (over z, y).
Axes of the slice: x: 4, y: 4, z: 4, core: 2. Of those that a mesh axis runs over, the one named last changes fastest.
Arguments:
- tail_vectors: float32 [64512, 4096], P('row', 'col'), may hold values from -6 to 6
- lower_panel: float32 [64512, 1024], P(('row', 'col')), may hold values from -0.0234375 to 0.0234375
- window_rhs: float32 [1024, 4096], P('row', 'col'), may hold values from -6 to 6
- window_block: float32 [1024, 1024], P(('row', 'col')), may hold values from -1 to 2, as said below
Outputs:
- window_vectors: float32 [1024, 4096], P('row', 'col')
The draws below stay inside these ranges and needn't reach their ends.
Inputs may be any that keep to these rules, and one draw needn't show every extreme that they name: window_block is zero above the diagonal; its diagonal lies in 1 to 2; entries below the diagonal are under 1 / sqrt(1024) in magnitude.
All inputs are finite; a program needn't handle non-finite values.
Results may differ from the reference program's by a relative error of at most 0.000082.
Values sent between devices are 32-bit elements; how exact they have to be, the bound alone decides.
A program may use at most 128 MiB of HBM per device.

```python
import jax
import jax.numpy as jnp
from jax import lax

NEV = 4096
WIN = 1024
TAIL = 64512


def draw_window_block(key, part):
    key_lower = jax.random.fold_in(key, 11)
    key_diag = jax.random.fold_in(key, 12)
    lower_mask = jnp.tril(jnp.ones((WIN, WIN), jnp.float32), -1)
    magnitude = 1.0 / jnp.sqrt(jnp.float32(WIN))
    spread = 0.98 * jax.random.uniform(key_lower, (WIN, WIN), jnp.float32, -1.0, 1.0)
    diagonal = jnp.exp(jax.random.uniform(key_diag, (WIN,), jnp.float32, 0.0, 0.69))
    return lower_mask * spread * magnitude + jnp.diag(diagonal)


def shard_levels(key, dims, cuts, smallest, high):
    factor_of, own = 1.0, jax.random.fold_in(key, 6)
    for position, parts in cuts:
        steps = jnp.exp(jax.random.uniform(jax.random.fold_in(own, position), (parts,), jnp.float32, smallest / len(cuts), high / len(cuts)))
        factor_of = factor_of * jnp.repeat(steps, dims[position] // parts).reshape([-1 if axis == position else 1 for axis in range(len(dims))])
    return factor_of


def centred(own_key, extent, scale, limit, shards=(), kind=jnp.bfloat16):
    drawn = jax.random.normal(own_key, extent, jnp.float32) * scale
    if len(shards) > 0:
        drawn = shard_levels(own_key, extent, shards, -0.22, 0.18) * drawn
    return jnp.clip(drawn, min=-limit, max=limit).astype(kind)


def setup_inputs(seed: int = 0) -> dict:
    key_list = jax.random.split(jax.random.key(seed), 5)
    return {
        "tail_vectors": centred(key_list[0], (TAIL, NEV), 1.0, 6.0, ((0, 8), (1, 16)), jnp.float32),
        "lower_panel": centred(key_list[1], (TAIL, WIN), TAIL ** -0.5, 0.0234375, ((0, 128),), jnp.float32),
        "window_rhs": centred(key_list[2], (WIN, NEV), 1.0, 6.0, ((0, 8), (1, 16)), jnp.float32),
        "window_block": draw_window_block(jax.random.fold_in(key_list[4], 71), 0),
    }


def reference(tail_vectors, lower_panel, window_rhs, window_block):
    correction = lax.dot_general(lower_panel.astype(jnp.float32), tail_vectors.astype(jnp.float32), (((0,), (0,)), ((), ())), precision=lax.Precision.HIGHEST, preferred_element_type=jnp.float32)
    right_side = window_rhs - correction
    return jax.scipy.linalg.solve_triangular(window_block, right_side, trans=1, lower=True)
```

```python
import functools

import jax
import jax.numpy as jnp
from jax import lax
from jax.experimental import pallas as pl
from jax.experimental.pallas import tpu as pltpu
from jax.sharding import PartitionSpec as P

MESH = pl.DeviceIdType.MESH
HIGHEST = lax.Precision.HIGHEST
F32 = jnp.float32
BF16 = jnp.bfloat16
SIDE = 4
PLACE = (0, 1, 3, 2)
PARTS = 3


def dot(a, b):
    return jnp.dot(a, b, precision=HIGHEST, preferred_element_type=F32)


def dot_t(a, b):
    return lax.dot_general(a, b, (((0,), (0,)), ((), ())), precision=HIGHEST, preferred_element_type=F32)


def mm(a, b):
    return jnp.dot(a, b, preferred_element_type=F32)


def halves(a):
    high = a.astype(BF16)
    return high, (a - high.astype(F32)).astype(BF16)


def lower_inverse(block, base=32):
    size = block.shape[0]
    rows = lax.broadcasted_iota(jnp.int32, (size, size), 0)
    cols = lax.broadcasted_iota(jnp.int32, (size, size), 1)
    eye = jnp.where(rows == cols, 1.0, 0.0)
    diag_col = jnp.sum(jnp.where(rows == cols, block, 0.0), axis=1, keepdims=True)
    diag_row = jnp.sum(jnp.where(rows == cols, block, 0.0), axis=0, keepdims=True)
    near = (rows // base == cols // base) & (rows > cols)
    power = jnp.where(near, -block / diag_col, 0.0)
    inverse = eye + power
    reach = 2
    while reach < base:
        power = dot(power, power)
        inverse = inverse + dot(inverse, power)
        reach *= 2
    inverse = inverse / diag_row
    while base < size:
        below = (rows // (2 * base) == cols // (2 * base)) & (rows // base > cols // base)
        inverse = inverse - dot(dot(inverse, jnp.where(below, block, 0.0)), inverse)
        base *= 2
    return inverse


def kernel(
    tail_hbm, panel_hbm, block_hbm, rhs_hbm, out_ref,
    tbuf, relay, pbuf, phi, plo, pthi, ptlo, wall, inv, inv_hi, inv_lo, tmp, rhs, thi, tlo,
    sums, core_in, first_in, second_in, last_in,
    local_sem, wz_s, wz_r, wy_s, wy_r, wa_s, wa_r, wb_s, wb_r, wc_s, wc_r,
    p_s, p_r, t_s, t_r, r_s, r_r, f_s, f_r,
    c_s, c_r, a_s, a_r, b_s, b_r, l_s, l_r,
):
    depth, window = panel_hbm.shape
    thin = block_hbm.shape[0]
    share, width = rhs_hbm.shape
    lane = width // 2
    pad = pbuf.shape[1]
    part = depth // PARTS
    r = lax.axis_index("row")
    c = lax.axis_index("col")
    x, k = r // 2, r % 2
    z, y = c // SIDE, c % SIDE
    step = 1 - 2 * k
    low, mirror = x + 1 - 2 * (x % 2), SIDE - 1 - x
    p1 = k * mirror + (1 - k) * low
    p2 = k * low + (1 - k) * mirror
    p12 = (x + 2) % SIDE

    def at_z(d):
        return {"col": ((z + d + SIDE) % SIDE) * SIDE + y}

    def at_y(d):
        return {"col": z * SIDE + (y + d + SIDE) % SIDE}

    def at_x(other):
        return {"row": 2 * other + k}

    partner = {"row": 2 * x + 1 - k}
    pending = []

    def remote(src, dst, send, recv, where):
        return pltpu.make_async_remote_copy(
            src_ref=src, dst_ref=dst, send_sem=send, recv_sem=recv, device_id=where, device_id_type=MESH
        )

    def go(src, dst, send, recv, where, keep=True):
        copy = remote(src, dst, send, recv, where)
        copy.start()
        if keep:
            pending.append(copy)
        return copy

    def arrived(dst, send, recv):
        remote(dst, dst, send, recv, partner).wait_recv()

    def owner_rows(dz, dy):
        owner = ((z + dz + SIDE) % SIDE) * SIDE + (y + dy) % SIDE
        return pl.ds(pl.multiple_of(owner * depth, 8), depth)

    def rows_of(index, size=128):
        return pl.ds(pl.multiple_of(index * size, size), size)

    own_thin = wall.at[r, pl.ds(pl.multiple_of(c * thin, 8), thin)]
    locals_ = [
        pltpu.make_async_copy(block_hbm, own_thin, local_sem.at[0]),
        pltpu.make_async_copy(panel_hbm, pbuf.at[0, pl.ds(0, depth)], local_sem.at[1]),
        pltpu.make_async_copy(rhs_hbm, rhs, local_sem.at[2]),
    ] + [
        pltpu.make_async_copy(tail_hbm.at[owner_rows(0, d)], tbuf.at[0, PLACE[d], pl.ds(0, depth)], local_sem.at[3 + d])
        for d in range(SIDE)
    ]
    for copy in locals_:
        copy.start()

    barrier = pltpu.get_barrier_semaphore()
    greeted = [at_z(d) for d in (1, 2, 3)] + [at_y(d) for d in (1, 2, 3)] + [at_x(p1), at_x(p2), partner]
    for where in greeted:
        pl.semaphore_signal(barrier, inc=1, device_id=where, device_id_type=MESH)
    pl.semaphore_wait(barrier, len(greeted))

    for d in (1, 3, 2):
        go(block_hbm, own_thin, wz_s.at[d], wz_r.at[SIDE - d], at_z(d))

    for d in (1, 3):
        for q in range(SIDE):
            go(tail_hbm.at[owner_rows(d, q)], tbuf.at[SIDE - d, PLACE[q], pl.ds(0, depth)],
               t_s.at[d, PLACE[q]], t_r.at[SIDE - d, PLACE[q]], at_z(d))
    for h in range(2):
        for q in range(SIDE):
            go(tail_hbm.at[owner_rows(2, q), pl.ds(h * lane, lane)], relay.at[h, PLACE[q]],
               r_s.at[h, PLACE[q]], r_r.at[h, PLACE[q]], at_z(step))

    zeros = jnp.zeros((pad - depth, width), F32)
    for j in range(SIDE):
        for q in range(SIDE):
            tbuf[j, q, pl.ds(depth, pad - depth), :] = zeros
    for q in range(SIDE):
        pbuf[q, pl.ds(depth, pad - depth), :] = jnp.zeros((pad - depth, window), F32)

    def thin_rows(zz, yy):
        return wall.at[r, pl.ds(pl.multiple_of((zz * SIDE + yy) * thin, 8), thin)]

    locals_[0].wait()
    for d in (1, 2, 3):
        dst = thin_rows((z + d) % SIDE, y)
        arrived(dst, wz_s.at[d], wz_r.at[d])
    thin_copies = []
    for d in (1, 3, 2):
        for zz in range(SIDE):
            thin_copies.append(go(thin_rows(zz, y), thin_rows(zz, y), wy_s.at[d, zz], wy_r.at[SIDE - d, zz], at_y(d), False))

    def part_rows(i):
        return pl.ds(i * part, part)

    for i in range(PARTS):
        go(panel_hbm.at[part_rows(i)], pbuf.at[2, part_rows(i)], p_s.at[0, i], p_r.at[2, i], at_y(1))
        go(panel_hbm.at[part_rows(i)], pbuf.at[1, part_rows(i)], p_s.at[1, i], p_r.at[1, i], at_y(3))

    for d in (1, 2, 3):
        for zz in range(SIDE):
            arrived(thin_rows(zz, (y + d) % SIDE), wy_s.at[d, zz], wy_r.at[d, zz])
    for copy in thin_copies:
        copy.wait_send()

    diag = rows_of(r, share)
    wall[r, :, diag] = lower_inverse(wall[r, :, diag])
    go(wall.at[r], wall.at[r], wa_s, wa_r, at_x(p2))
    arrived(wall.at[2 * p2 + k], wa_s, wa_r)
    go(wall.at[r], wall.at[r], wb_s.at[0], wb_r.at[0], at_x(p1))
    go(wall.at[2 * p2 + k], wall.at[2 * p2 + k], wb_s.at[1], wb_r.at[1], at_x(p1))
    arrived(wall.at[2 * p1 + k], wb_s.at[0], wb_r.at[0])
    arrived(wall.at[2 * p12 + k], wb_s.at[1], wb_r.at[1])
    for i in range(SIDE):
        go(wall.at[2 * i + k], wall.at[2 * i + k], wc_s.at[i], wc_r.at[i], partner)

    near = 2 - k

    def pass_panel(i):
        arrived(pbuf.at[near, part_rows(i)], p_s.at[2, i], p_r.at[near, i])
        go(pbuf.at[near, part_rows(i)], pbuf.at[3, part_rows(i)], p_s.at[2, i], p_r.at[3, i], at_y(step))

    pass_panel(0)
    for i in range(SIDE):
        arrived(wall.at[2 * i + 1 - k], wc_s.at[i], wc_r.at[i])
    pass_panel(1)

    def clear(i, _):
        inv[rows_of(i), :] = jnp.zeros((128, window), F32)
        return 0

    blocks = window // share
    lax.fori_loop(0, window // 128, clear, 0)
    for i in range(blocks):
        inv[pl.ds(i * share, share), pl.ds(i * share, share)] = wall[i, :, pl.ds(i * share, share)]
    size = share
    while size < window:
        count = size // share
        strip = min(size, 256)
        for base in range(0, window, 2 * size):
            top, low_rows = pl.ds(base, size), pl.ds(base + size, size)

            def below(i, _, base=base, size=size, count=count, strip=strip, top=top, low_rows=low_rows):
                start = pl.multiple_of(i * strip, strip)
                left = inv[pl.ds(base + size + start, strip), low_rows]
                under = wall[pl.ds(base // share + count, count), :, top].reshape(size, size)
                tmp[pl.ds(0, strip), pl.ds(0, size)] = dot(left, under)
                inv[pl.ds(base + size + start, strip), top] = -dot(tmp[pl.ds(0, strip), pl.ds(0, size)], inv[top, top])
                return 0

            if strip == size:
                below(0, 0)
            else:
                lax.fori_loop(0, size // strip, below, 0)
        size *= 2

    def split_inverse(i, _):
        high, rest = halves(inv[rows_of(i), :])
        inv_hi[rows_of(i), :] = high
        inv_lo[rows_of(i), :] = rest
        return 0

    lax.fori_loop(0, window // 128, split_inverse, 0)
    pass_panel(2)

    def turn_panel(q, _):
        def split_rows(i, _):
            high, rest = halves(pbuf[q, rows_of(i), :])
            phi[rows_of(i), :] = high
            plo[rows_of(i), :] = rest
            return 0

        lax.fori_loop(0, pad // 128, split_rows, 0)
        place = pl.ds(pl.multiple_of(q * pad, pad), pad)
        for n in range(0, window, 256):
            deep, cols = pl.ds(n, window - n), pl.ds(n, 256)
            product = (
                mm(phi[:, deep], inv_hi[deep, cols])
                + mm(phi[:, deep], inv_lo[deep, cols])
                + mm(plo[:, deep], inv_hi[deep, cols])
            )
            high, rest = halves(-product.T)
            pthi[cols, place] = high
            ptlo[cols, place] = rest
        return 0

    def panel_here(q):
        for i in range(PARTS):
            arrived(pbuf.at[q, part_rows(i)], p_s.at[0, i], p_r.at[q, i])

    locals_[1].wait()
    for i in range(PARTS):
        arrived(pbuf.at[3 - near, part_rows(i)], p_s.at[0, i], p_r.at[3 - near, i])
    lax.fori_loop(0, 3, turn_panel, 0)

    def take_tail(j, places, cols):
        for q in places:
            high, rest = halves(tbuf[j, q, :, cols])
            thi[pl.ds(q * pad, pad), cols] = high
            tlo[pl.ds(q * pad, pad), cols] = rest

    strip = 512

    def product(j, places, cols, fresh):
        take_tail(j, places, cols)
        deep = pl.ds(places[0] * pad, len(places) * pad)

        def one(i, _):
            rows = rows_of(i, strip)
            total = (
                mm(pthi[rows, deep], thi[deep, cols])
                + mm(pthi[rows, deep], tlo[deep, cols])
                + mm(ptlo[rows, deep], thi[deep, cols])
            )
            for h in range(total.shape[1] // lane):
                u = 2 * j + h + cols.start // lane
                piece = total[:, h * lane:(h + 1) * lane]
                sums[u, rows, :] = piece if fresh else sums[u, rows, :] + piece
            return 0

        lax.fori_loop(0, window // strip, one, 0)

    whole = pl.ds(0, width)
    early = (0, 1, 2)

    def tail_here(j):
        for q in range(SIDE):
            arrived(tbuf.at[j, q, pl.ds(0, depth)], t_s.at[1, q], t_r.at[j, q])

    for copy in locals_[2:]:
        copy.wait()
    product(0, early, whole, True)
    own = dot_t(inv[rows_of(r, share), :], rhs[...])
    for h in range(2):
        sums[h] = sums[h] + own[:, h * lane:(h + 1) * lane]
    tail_here(1)
    product(1, early, whole, True)
    tail_here(3)
    product(3, early, whole, True)

    def pass_tail(h):
        for q in range(SIDE):
            q = PLACE[q]
            arrived(relay.at[h, q], r_s.at[h, q], r_r.at[h, q])
            go(relay.at[h, q], tbuf.at[2, q, pl.ds(0, depth), pl.ds(h * lane, lane)],
               f_s.at[h, q], f_r.at[h, q], at_z(step))

    pass_tail(0)
    panel_here(3)
    turn_panel(3, 0)

    def line(u, rr):
        return sums.at[u, rows_of(rr, share)]

    def to_core(u):
        for i in range(SIDE):
            go(line(u, 2 * i + 1 - k), core_in.at[u, i], c_s.at[u, i], c_r.at[u, i], partner)

    def to_first(u):
        for i in range(SIDE):
            arrived(core_in.at[u, i], c_s.at[u, i], c_r.at[u, i])
            rows = rows_of(2 * i + k, share)
            sums[u, rows, :] = sums[u, rows, :] + core_in[u, i]
        go(line(u, 2 * p1 + k), first_in.at[u, 0], a_s.at[u, 0], a_r.at[u, 0], at_x(p1))
        go(line(u, 2 * p12 + k), first_in.at[u, 1], a_s.at[u, 1], a_r.at[u, 1], at_x(p1))

    def to_second(u):
        for i, other in ((1, p2), (0, x)):
            arrived(first_in.at[u, i], a_s.at[u, i], a_r.at[u, i])
            rows = rows_of(2 * other + k, share)
            sums[u, rows, :] = sums[u, rows, :] + first_in[u, i]
            if i == 1:
                go(line(u, 2 * p2 + k), second_in.at[u], b_s.at[u], b_r.at[u], at_x(p2))

    def to_last(u):
        j, h = u // 2, u % 2
        arrived(second_in.at[u], b_s.at[u], b_r.at[u])
        rows = rows_of(r, share)
        sums[u, rows, :] = sums[u, rows, :] + second_in[u]
        if j:
            go(line(u, r), last_in.at[SIDE - j, h], l_s.at[u], l_r.at[SIDE - j, h], at_z(j))

    def both(stage, j):
        stage(2 * j)
        stage(2 * j + 1)

    late = (3,)
    product(0, late, whole, False)
    both(to_core, 0)
    product(1, late, whole, False)
    both(to_core, 1)
    both(to_first, 0)
    product(3, late, whole, False)
    both(to_core, 3)
    both(to_first, 1)
    both(to_second, 0)
    pass_tail(1)
    both(to_first, 3)
    both(to_second, 1)
    both(to_last, 0)

    def cross_here(h):
        for q in range(SIDE):
            arrived(tbuf.at[2, q, pl.ds(0, depth), pl.ds(h * lane, lane)], f_s.at[h, q], f_r.at[h, q])

    every = (0, 1, 2, 3)
    cross_here(0)
    product(2, every, pl.ds(0, lane), True)
    to_core(4)
    both(to_second, 3)
    both(to_last, 1)
    to_first(4)
    both(to_last, 3)
    cross_here(1)
    product(2, every, pl.ds(lane, lane), True)
    to_core(5)
    to_second(4)
    to_first(5)
    to_last(4)
    to_second(5)
    to_last(5)

    rows = rows_of(r, share)
    for h in range(2):
        total = sums[h, rows, :]
        for d in (1, 3, 2):
            arrived(last_in.at[d, h], l_s.at[2 + h], l_r.at[d, h])
            total = total + last_in[d, h]
        out_ref[:, h * lane:(h + 1) * lane] = total

    for copy in pending:
        copy.wait_send()


def per_device(tail_vectors, lower_panel, window_rhs, window_block):
    columns = tail_vectors.shape[1]
    depth, window = lower_panel.shape
    share = window_rhs.shape[0]
    lane = columns // 2
    pad = -(-depth // 128) * 128
    groups = window // share
    dma = pltpu.SemaphoreType.DMA
    anywhere = pl.BlockSpec(memory_space=pl.ANY)
    return pl.pallas_call(
        kernel,
        out_shape=jax.ShapeDtypeStruct((share, columns), F32),
        in_specs=[anywhere] * 4,
        out_specs=pl.BlockSpec(memory_space=pltpu.VMEM),
        scratch_shapes=[
            pltpu.VMEM((SIDE, SIDE, pad, columns), F32),
            pltpu.VMEM((2, SIDE, depth, lane), F32),
            pltpu.VMEM((SIDE, pad, window), F32),
            pltpu.VMEM((pad, window), BF16),
            pltpu.VMEM((pad, window), BF16),
            pltpu.VMEM((window, SIDE * pad), BF16),
            pltpu.VMEM((window, SIDE * pad), BF16),
            pltpu.VMEM((groups, share, window), F32),
            pltpu.VMEM((window, window), F32),
            pltpu.VMEM((window, window), BF16),
            pltpu.VMEM((window, window), BF16),
            pltpu.VMEM((256, window // 2), F32),
            pltpu.VMEM((share, columns), F32),
            pltpu.VMEM((SIDE * pad, columns), BF16),
            pltpu.VMEM((SIDE * pad, columns), BF16),
            pltpu.VMEM((2 * SIDE, window, lane), F32),
            pltpu.VMEM((2 * SIDE, SIDE, share, lane), F32),
            pltpu.VMEM((2 * SIDE, 2, share, lane), F32),
            pltpu.VMEM((2 * SIDE, share, lane), F32),
            pltpu.VMEM((SIDE, 2, share, lane), F32),
            dma((7,)),
            dma((SIDE,)), dma((SIDE,)), dma((SIDE, SIDE)), dma((SIDE, SIDE)),
            dma, dma, dma((2,)), dma((2,)), dma((SIDE,)), dma((SIDE,)),
            dma((3, PARTS)), dma((SIDE, PARTS)),
            dma((SIDE, SIDE)), dma((SIDE, SIDE)),
            dma((2, SIDE)), dma((2, SIDE)), dma((2, SIDE)), dma((2, SIDE)),
            dma((2 * SIDE, SIDE)), dma((2 * SIDE, SIDE)),
            dma((2 * SIDE, 2)), dma((2 * SIDE, 2)),
            dma((2 * SIDE,)), dma((2 * SIDE,)),
            dma((2 * SIDE,)), dma((SIDE, 2)),
        ],
        compiler_params=pltpu.CompilerParams(
            collective_id=0, has_side_effects=True, vmem_limit_bytes=65000 * 1024
        ),
    )(tail_vectors, lower_panel, window_block, window_rhs)


def solution(mesh):
    in_specs = (P("row", "col"), P(("row", "col"), None), P("row", "col"), P(("row", "col"), None))
    out_specs = P("row", "col")
    return jax.shard_map(per_device, mesh=mesh, in_specs=in_specs, out_specs=out_specs, check_vma=False)
```

```python
import functools

import jax
import jax.numpy as jnp
from jax import lax
from jax.experimental import pallas as pl
from jax.experimental.pallas import tpu as pltpu
from jax.sharding import PartitionSpec as P

MESH = pl.DeviceIdType.MESH
HIGHEST = lax.Precision.HIGHEST
F32 = jnp.float32
BF16 = jnp.bfloat16
SIDE = 4
PLACE = (0, 1, 3, 2)
CUTS = (3, 5, 11, 11, 11, 11, 11)
PARTS = len(CUTS)


def dot(a, b):
    return jnp.dot(a, b, precision=HIGHEST, preferred_element_type=F32)


def dot_t(a, b):
    return lax.dot_general(a, b, (((0,), (0,)), ((), ())), precision=HIGHEST, preferred_element_type=F32)


def mm(a, b):
    return jnp.dot(a, b, preferred_element_type=F32)


def halves(a):
    high = a.astype(BF16)
    return high, (a - high.astype(F32)).astype(BF16)


def lower_inverse(block, base=32):
    size = block.shape[0]
    rows = lax.broadcasted_iota(jnp.int32, (size, size), 0)
    cols = lax.broadcasted_iota(jnp.int32, (size, size), 1)
    eye = jnp.where(rows == cols, 1.0, 0.0)
    diag_col = jnp.sum(jnp.where(rows == cols, block, 0.0), axis=1, keepdims=True)
    diag_row = jnp.sum(jnp.where(rows == cols, block, 0.0), axis=0, keepdims=True)
    near = (rows // base == cols // base) & (rows > cols)
    power = jnp.where(near, -block / diag_col, 0.0)
    inverse = eye + power
    reach = 2
    while reach < base:
        power = dot(power, power)
        inverse = inverse + dot(inverse, power)
        reach *= 2
    inverse = inverse / diag_row
    while base < size:
        below = (rows // (2 * base) == cols // (2 * base)) & (rows // base > cols // base)
        inverse = inverse - dot(dot(inverse, jnp.where(below, block, 0.0)), inverse)
        base *= 2
    return inverse


def kernel(
    tail_hbm, panel_hbm, block_hbm, rhs_hbm, out_ref,
    tbuf, relay, pbuf, phi, plo, pthi, ptlo, wall, inv, inv_hi, inv_lo, tmp, rhs, thi, tlo,
    sums, core_in, first_in, second_in, last_in,
    local_sem, wz_s, wz_r, wy_s, wy_r, wa_s, wa_r, wb_s, wb_r, wc_s, wc_r,
    p_s, p_r, t_s, t_r, r_s, r_r, f_s, f_r,
    c_s, c_r, a_s, a_r, b_s, b_r, l_s, l_r,
):
    depth, window = panel_hbm.shape
    thin = block_hbm.shape[0]
    share, width = rhs_hbm.shape
    lane = width // 2
    pad = pbuf.shape[1]
    unit = depth // sum(CUTS)
    r = lax.axis_index("row")
    c = lax.axis_index("col")
    x, k = r // 2, r % 2
    z, y = c // SIDE, c % SIDE
    step = 1 - 2 * k
    low, mirror = x + 1 - 2 * (x % 2), SIDE - 1 - x
    p1 = k * mirror + (1 - k) * low
    p2 = k * low + (1 - k) * mirror
    p12 = (x + 2) % SIDE
    low, mirror = y + 1 - 2 * (y % 2), SIDE - 1 - y
    q1 = k * mirror + (1 - k) * low
    q2 = k * low + (1 - k) * mirror
    q12 = (y + 2) % SIDE

    def at_z(d):
        return {"col": ((z + d + SIDE) % SIDE) * SIDE + y}

    def at_y(d):
        return {"col": z * SIDE + (y + d + SIDE) % SIDE}

    def at_x(other):
        return {"row": 2 * other + k}

    partner = {"row": 2 * x + 1 - k}
    pending = []

    def remote(src, dst, send, recv, where):
        return pltpu.make_async_remote_copy(
            src_ref=src, dst_ref=dst, send_sem=send, recv_sem=recv, device_id=where, device_id_type=MESH
        )

    def go(src, dst, send, recv, where, keep=True):
        copy = remote(src, dst, send, recv, where)
        copy.start()
        if keep:
            pending.append(copy)
        return copy

    def arrived(dst, send, recv):
        remote(dst, dst, send, recv, partner).wait_recv()

    def owner_rows(dz, dy):
        owner = ((z + dz + SIDE) % SIDE) * SIDE + (y + dy) % SIDE
        return pl.ds(pl.multiple_of(owner * depth, 8), depth)

    def rows_of(index, size=128):
        return pl.ds(pl.multiple_of(index * size, size), size)

    own_thin = wall.at[r, pl.ds(pl.multiple_of(c * thin, 8), thin)]
    locals_ = [
        pltpu.make_async_copy(block_hbm, own_thin, local_sem.at[0]),
        pltpu.make_async_copy(panel_hbm, pbuf.at[0, pl.ds(0, depth)], local_sem.at[1]),
        pltpu.make_async_copy(rhs_hbm, rhs, local_sem.at[2]),
    ] + [
        pltpu.make_async_copy(tail_hbm.at[owner_rows(0, d)], tbuf.at[0, PLACE[d], pl.ds(0, depth)], local_sem.at[3 + d])
        for d in range(SIDE)
    ]
    for copy in locals_:
        copy.start()

    barrier = pltpu.get_barrier_semaphore()
    greeted = [at_z(d) for d in (1, 2, 3)] + [at_y(1), at_y(3)] + [at_x(p1), at_x(p2), partner]
    for where in greeted:
        pl.semaphore_signal(barrier, inc=1, device_id=where, device_id_type=MESH)
    pl.semaphore_wait(barrier, len(greeted))

    def part_rows(i):
        return pl.ds(sum(CUTS[:i]) * unit, CUTS[i] * unit)

    def send_panel(i):
        go(panel_hbm.at[part_rows(i)], pbuf.at[2, part_rows(i)], p_s.at[0, i], p_r.at[2, i], at_y(1))
        go(panel_hbm.at[part_rows(i)], pbuf.at[1, part_rows(i)], p_s.at[1, i], p_r.at[1, i], at_y(3))

    for d in (2, 1, 3):
        go(block_hbm, own_thin, wz_s.at[d], wz_r.at[SIDE - d], at_z(d))
    send_panel(0)

    for h in range(2):
        for q in (0, 1, 3, 2):
            go(tail_hbm.at[owner_rows(2, q), pl.ds(h * lane, lane)], relay.at[h, PLACE[q]],
               r_s.at[h, PLACE[q]], r_r.at[h, PLACE[q]], at_z(step))
    for d in (1, 3):
        for q in range(SIDE):
            go(tail_hbm.at[owner_rows(d, q)], tbuf.at[SIDE - d, PLACE[q], pl.ds(0, depth)],
               t_s.at[d, PLACE[q]], t_r.at[SIDE - d, PLACE[q]], at_z(d))

    zeros = jnp.zeros((pad - depth, width), F32)
    for j in range(SIDE):
        for q in range(SIDE):
            tbuf[j, q, pl.ds(depth, pad - depth), :] = zeros
    for q in range(SIDE):
        pbuf[q, pl.ds(depth, pad - depth), :] = jnp.zeros((pad - depth, window), F32)

    def thin_rows(zz, yy):
        return wall.at[r, pl.ds(pl.multiple_of((zz * SIDE + yy) * thin, 8), thin)]

    def here_y(other):
        return {"col": z * SIDE + other}

    locals_[0].wait()
    for d in (1, 3, 2):
        dst = thin_rows((z + d) % SIDE, y)
        arrived(dst, wz_s.at[d], wz_r.at[d])
    thin_copies = []

    def swap_thin(sem, mine, where):
        for zz in range(SIDE):
            thin_copies.append(
                go(thin_rows(zz, mine), thin_rows(zz, mine), wy_s.at[sem, zz], wy_r.at[sem, zz], here_y(where), False)
            )

    def thin_here(sem, theirs):
        for zz in range(SIDE):
            arrived(thin_rows(zz, theirs), wy_s.at[sem, zz], wy_r.at[sem, zz])

    swap_thin(0, y, q1)
    send_panel(1)
    thin_here(0, q1)
    swap_thin(1, y, q2)
    swap_thin(2, q1, q2)
    for i in range(2, PARTS):
        send_panel(i)
    thin_here(1, q2)
    thin_here(2, q12)
    for copy in thin_copies:
        copy.wait_send()

    diag = rows_of(r, share)
    wall[r, :, diag] = lower_inverse(wall[r, :, diag])
    near = 2 - k

    def pass_panel(i):
        arrived(pbuf.at[near, part_rows(i)], p_s.at[2, i], p_r.at[near, i])
        go(pbuf.at[near, part_rows(i)], pbuf.at[3, part_rows(i)], p_s.at[2, i], p_r.at[3, i], at_y(step))

    def strip_to_core(i, other):
        go(wall.at[2 * other + k], wall.at[2 * other + k], wc_s.at[i], wc_r.at[i], partner)

    go(wall.at[r], wall.at[r], wa_s, wa_r, at_x(p2))
    go(wall.at[r], wall.at[r], wb_s.at[0], wb_r.at[0], at_x(p1))
    strip_to_core(0, x)
    pass_panel(0)
    pass_panel(1)
    arrived(wall.at[2 * p2 + k], wa_s, wa_r)
    go(wall.at[2 * p2 + k], wall.at[2 * p2 + k], wb_s.at[1], wb_r.at[1], at_x(p1))
    strip_to_core(1, p2)
    arrived(wall.at[2 * p1 + k], wb_s.at[0], wb_r.at[0])
    strip_to_core(2, p1)
    pass_panel(2)
    pass_panel(3)
    arrived(wall.at[2 * p12 + k], wb_s.at[1], wb_r.at[1])
    strip_to_core(3, p12)
    pass_panel(4)
    for i, other in enumerate((x, p1, p2, p12)):
        arrived(wall.at[2 * other + 1 - k], wc_s.at[i], wc_r.at[i])

    def clear(i, _):
        inv[rows_of(i), :] = jnp.zeros((128, window), F32)
        return 0

    blocks = window // share
    lax.fori_loop(0, window // 128, clear, 0)
    for i in range(blocks):
        inv[pl.ds(i * share, share), pl.ds(i * share, share)] = wall[i, :, pl.ds(i * share, share)]
    size = share
    while size < window:
        count = size // share
        strip = min(size, 256)
        for base in range(0, window, 2 * size):
            top, low_rows = pl.ds(base, size), pl.ds(base + size, size)

            def below(i, _, base=base, size=size, count=count, strip=strip, top=top, low_rows=low_rows):
                start = pl.multiple_of(i * strip, strip)
                left = inv[pl.ds(base + size + start, strip), low_rows]
                under = wall[pl.ds(base // share + count, count), :, top].reshape(size, size)
                tmp[pl.ds(0, strip), pl.ds(0, size)] = dot(left, under)
                inv[pl.ds(base + size + start, strip), top] = -dot(tmp[pl.ds(0, strip), pl.ds(0, size)], inv[top, top])
                return 0

            if strip == size:
                below(0, 0)
            else:
                lax.fori_loop(0, size // strip, below, 0)
        size *= 2

    def split_inverse(i, _):
        high, rest = halves(inv[rows_of(i), :])
        inv_hi[rows_of(i), :] = high
        inv_lo[rows_of(i), :] = rest
        return 0

    lax.fori_loop(0, window // 128, split_inverse, 0)

    def pass_tail(h):
        for q in range(SIDE):
            arrived(relay.at[h, q], r_s.at[h, q], r_r.at[h, q])
            go(relay.at[h, q], tbuf.at[2, q, pl.ds(0, depth), pl.ds(h * lane, lane)],
               f_s.at[h, q], f_r.at[h, q], at_z(step))

    def turn_panel(q, _):
        def split_rows(i, _):
            high, rest = halves(pbuf[q, rows_of(i), :])
            phi[rows_of(i), :] = high
            plo[rows_of(i), :] = rest
            return 0

        lax.fori_loop(0, pad // 128, split_rows, 0)
        place = pl.ds(pl.multiple_of(q * pad, pad), pad)
        for n in range(0, window, 256):
            deep, cols = pl.ds(n, window - n), pl.ds(n, 256)
            product = (
                mm(phi[:, deep], inv_hi[deep, cols])
                + mm(phi[:, deep], inv_lo[deep, cols])
                + mm(plo[:, deep], inv_hi[deep, cols])
            )
            high, rest = halves(-product.T)
            pthi[cols, place] = high
            ptlo[cols, place] = rest
        return 0

    def panel_here(q):
        for i in range(PARTS):
            arrived(pbuf.at[q, part_rows(i)], p_s.at[0, i], p_r.at[q, i])

    locals_[1].wait()
    turn_panel(0, 0)
    pass_panel(5)
    pass_panel(6)
    pass_tail(0)
    for i in range(PARTS):
        arrived(pbuf.at[3 - near, part_rows(i)], p_s.at[0, i], p_r.at[3 - near, i])
    lax.fori_loop(1, 3, turn_panel, 0)
    pass_tail(1)

    def take_tail(j, places, cols):
        for q in places:
            high, rest = halves(tbuf[j, q, :, cols])
            thi[pl.ds(q * pad, pad), cols] = high
            tlo[pl.ds(q * pad, pad), cols] = rest

    strip = 512

    def product(j, places, cols, fresh):
        take_tail(j, places, cols)
        deep = pl.ds(places[0] * pad, len(places) * pad)

        def one(i, _):
            rows = rows_of(i, strip)
            total = (
                mm(pthi[rows, deep], thi[deep, cols])
                + mm(pthi[rows, deep], tlo[deep, cols])
                + mm(ptlo[rows, deep], thi[deep, cols])
            )
            for h in range(total.shape[1] // lane):
                u = 2 * j + h + cols.start // lane
                piece = total[:, h * lane:(h + 1) * lane]
                sums[u, rows, :] = piece if fresh else sums[u, rows, :] + piece
            return 0

        lax.fori_loop(0, window // strip, one, 0)

    whole = pl.ds(0, width)
    early = (0, 1, 2)

    def tail_here(j, places):
        for q in places:
            arrived(tbuf.at[j, q, pl.ds(0, depth)], t_s.at[1, q], t_r.at[j, q])

    late = (3,)
    for copy in locals_[2:]:
        copy.wait()
    product(0, early, whole, True)
    own = dot_t(inv[rows_of(r, share), :], rhs[...])
    for h in range(2):
        sums[h] = sums[h] + own[:, h * lane:(h + 1) * lane]
    for j in (1 + 2 * k, 3 - 2 * k):
        tail_here(j, early)
        product(j, early, whole, True)

    panel_here(3)
    turn_panel(3, 0)

    def line(u, rr):
        return sums.at[u, rows_of(rr, share)]

    def to_core(u):
        for i in range(SIDE):
            go(line(u, 2 * i + 1 - k), core_in.at[u, i], c_s.at[u, i], c_r.at[u, i], partner)

    def to_first(u):
        for i in range(SIDE):
            arrived(core_in.at[u, i], c_s.at[u, i], c_r.at[u, i])
            rows = rows_of(2 * i + k, share)
            sums[u, rows, :] = sums[u, rows, :] + core_in[u, i]
        go(line(u, 2 * p1 + k), first_in.at[u, 0], a_s.at[u, 0], a_r.at[u, 0], at_x(p1))
        go(line(u, 2 * p12 + k), first_in.at[u, 1], a_s.at[u, 1], a_r.at[u, 1], at_x(p1))

    def to_second(u):
        for i, other in ((1, p2), (0, x)):
            arrived(first_in.at[u, i], a_s.at[u, i], a_r.at[u, i])
            rows = rows_of(2 * other + k, share)
            sums[u, rows, :] = sums[u, rows, :] + first_in[u, i]
            if i == 1:
                go(line(u, 2 * p2 + k), second_in.at[u], b_s.at[u], b_r.at[u], at_x(p2))

    def to_last(u):
        j, h = u // 2, u % 2
        arrived(second_in.at[u], b_s.at[u], b_r.at[u])
        rows = rows_of(r, share)
        sums[u, rows, :] = sums[u, rows, :] + second_in[u]
        if j:
            go(line(u, r), last_in.at[SIDE - j, h], l_s.at[u], l_r.at[SIDE - j, h], at_z(j))

    def both(stage, j):
        stage(2 * j)
        stage(2 * j + 1)

    def cross(h, places, fresh):
        for q in places:
            arrived(tbuf.at[2, q, pl.ds(0, depth), pl.ds(h * lane, lane)], f_s.at[h, q], f_r.at[h, q])
        product(2, places, pl.ds(h * lane, lane), fresh)

    product(0, late, whole, False)
    both(to_core, 0)
    tail_here(1, late)
    product(1, late, whole, False)
    both(to_core, 1)
    both(to_first, 0)
    tail_here(3, late)
    product(3, late, whole, False)
    both(to_core, 3)
    both(to_first, 1)
    cross(0, (0, 1), True)
    both(to_first, 3)
    both(to_second, 0)
    cross(0, (2, 3), False)
    to_core(4)
    both(to_second, 1)
    to_first(4)
    cross(1, (0, 1), True)
    both(to_last, 0)
    both(to_second, 3)
    both(to_last, 1)
    cross(1, (2,), False)
    to_second(4)
    both(to_last, 3)
    cross(1, (3,), False)
    to_core(5)
    to_first(5)
    to_last(4)
    to_second(5)
    to_last(5)

    rows = rows_of(r, share)
    for h in range(2):
        total = sums[h, rows, :]
        for d in (1, 3, 2):
            arrived(last_in.at[d, h], l_s.at[2 + h], l_r.at[d, h])
            total = total + last_in[d, h]
        out_ref[:, h * lane:(h + 1) * lane] = total

    for copy in pending:
        copy.wait_send()


def per_device(tail_vectors, lower_panel, window_rhs, window_block):
    columns = tail_vectors.shape[1]
    depth, window = lower_panel.shape
    share = window_rhs.shape[0]
    lane = columns // 2
    pad = -(-depth // 128) * 128
    groups = window // share
    dma = pltpu.SemaphoreType.DMA
    anywhere = pl.BlockSpec(memory_space=pl.ANY)
    return pl.pallas_call(
        kernel,
        out_shape=jax.ShapeDtypeStruct((share, columns), F32),
        in_specs=[anywhere] * 4,
        out_specs=pl.BlockSpec(memory_space=pltpu.VMEM),
        scratch_shapes=[
            pltpu.VMEM((SIDE, SIDE, pad, columns), F32),
            pltpu.VMEM((2, SIDE, depth, lane), F32),
            pltpu.VMEM((SIDE, pad, window), F32),
            pltpu.VMEM((pad, window), BF16),
            pltpu.VMEM((pad, window), BF16),
            pltpu.VMEM((window, SIDE * pad), BF16),
            pltpu.VMEM((window, SIDE * pad), BF16),
            pltpu.VMEM((groups, share, window), F32),
            pltpu.VMEM((window, window), F32),
            pltpu.VMEM((window, window), BF16),
            pltpu.VMEM((window, window), BF16),
            pltpu.VMEM((256, window // 2), F32),
            pltpu.VMEM((share, columns), F32),
            pltpu.VMEM((SIDE * pad, columns), BF16),
            pltpu.VMEM((SIDE * pad, columns), BF16),
            pltpu.VMEM((2 * SIDE, window, lane), F32),
            pltpu.VMEM((2 * SIDE, SIDE, share, lane), F32),
            pltpu.VMEM((2 * SIDE, 2, share, lane), F32),
            pltpu.VMEM((2 * SIDE, share, lane), F32),
            pltpu.VMEM((SIDE, 2, share, lane), F32),
            dma((7,)),
            dma((SIDE,)), dma((SIDE,)), dma((3, SIDE)), dma((3, SIDE)),
            dma, dma, dma((2,)), dma((2,)), dma((SIDE,)), dma((SIDE,)),
            dma((3, PARTS)), dma((SIDE, PARTS)),
            dma((SIDE, SIDE)), dma((SIDE, SIDE)),
            dma((2, SIDE)), dma((2, SIDE)), dma((2, SIDE)), dma((2, SIDE)),
            dma((2 * SIDE, SIDE)), dma((2 * SIDE, SIDE)),
            dma((2 * SIDE, 2)), dma((2 * SIDE, 2)),
            dma((2 * SIDE,)), dma((2 * SIDE,)),
            dma((2 * SIDE,)), dma((SIDE, 2)),
        ],
        compiler_params=pltpu.CompilerParams(
            collective_id=0, has_side_effects=True, vmem_limit_bytes=65000 * 1024
        ),
    )(tail_vectors, lower_panel, window_block, window_rhs)


def solution(mesh):
    in_specs = (P("row", "col"), P(("row", "col"), None), P("row", "col"), P(("row", "col"), None))
    out_specs = P("row", "col")
    return jax.shard_map(per_device, mesh=mesh, in_specs=in_specs, out_specs=out_specs, check_vma=False)
```

```python
import functools

import jax
import jax.numpy as jnp
from jax import lax
from jax.experimental import pallas as pl
from jax.experimental.pallas import tpu as pltpu
from jax.sharding import PartitionSpec as P

MESH = pl.DeviceIdType.MESH
HIGHEST = lax.Precision.HIGHEST
F32 = jnp.float32
BF16 = jnp.bfloat16
SIDE = 4
PLACE = (0, 1, 3, 2)
CUTS = (9, 6, 8, 8, 8, 12, 12)
PARTS = len(CUTS)
FORTH = 4


def dot(a, b):
    return jnp.dot(a, b, precision=HIGHEST, preferred_element_type=F32)


def mm_t(a, b):
    return lax.dot_general(a, b, (((0,), (0,)), ((), ())), preferred_element_type=F32)


def mm(a, b):
    return jnp.dot(a, b, preferred_element_type=F32)


def halves(a):
    high = a.astype(BF16)
    return high, (a - high.astype(F32)).astype(BF16)


def lower_inverse(block, base=32):
    size = block.shape[0]
    rows = lax.broadcasted_iota(jnp.int32, (size, size), 0)
    cols = lax.broadcasted_iota(jnp.int32, (size, size), 1)
    eye = jnp.where(rows == cols, 1.0, 0.0)
    diag_col = jnp.sum(jnp.where(rows == cols, block, 0.0), axis=1, keepdims=True)
    diag_row = jnp.sum(jnp.where(rows == cols, block, 0.0), axis=0, keepdims=True)
    near = (rows // base == cols // base) & (rows > cols)
    power = jnp.where(near, -block / diag_col, 0.0)
    inverse = eye + power
    reach = 2
    while reach < base:
        power = dot(power, power)
        inverse = inverse + dot(inverse, power)
        reach *= 2
    inverse = inverse / diag_row
    while base < size:
        below = (rows // (2 * base) == cols // (2 * base)) & (rows // base > cols // base)
        inverse = inverse - dot(dot(inverse, jnp.where(below, block, 0.0)), inverse)
        base *= 2
    return inverse


def kernel(
    tail_hbm, panel_hbm, block_hbm, rhs_hbm, out_ref,
    tbuf, relay, pbuf, phi, plo, pthi, ptlo, wall, inv, inv_hi, inv_lo, tmp, rhs, thi, tlo,
    sums, core_in, first_in, second_in, last_in,
    local_sem, wz_s, wz_r, wy_s, wy_r, wa_s, wa_r, wb_s, wb_r, wc_s, wc_r,
    p_s, p_r, t_s, t_r, r_s, r_r, f_s, f_r,
    c_s, c_r, a_s, a_r, b_s, b_r, l_s, l_r,
):
    depth, window = panel_hbm.shape
    thin = block_hbm.shape[0]
    share, width = rhs_hbm.shape
    lane = width // 2
    pad = pbuf.shape[1]
    unit = depth // sum(CUTS)
    r = lax.axis_index("row")
    c = lax.axis_index("col")
    x, k = r // 2, r % 2
    z, y = c // SIDE, c % SIDE
    low, mirror = x + 1 - 2 * (x % 2), SIDE - 1 - x
    p1 = k * mirror + (1 - k) * low
    p2 = k * low + (1 - k) * mirror
    p12 = (x + 2) % SIDE

    def place_at(dt, dp):
        zz = (z + dt * (1 - k) + dp * k + 2 * SIDE) % SIDE
        yy = (y + dt * k + dp * (1 - k) + 2 * SIDE) % SIDE
        return zz * SIDE + yy

    def at_t(d):
        return {"row": r, "col": place_at(d, 0)}

    def at_p(d):
        return {"row": r, "col": place_at(0, d)}

    def at_x(other):
        return {"row": 2 * other + k, "col": c}

    partner = {"row": 2 * x + 1 - k, "col": c}
    pending = []

    def remote(src, dst, send, recv, where):
        return pltpu.make_async_remote_copy(
            src_ref=src, dst_ref=dst, send_sem=send, recv_sem=recv, device_id=where, device_id_type=MESH
        )

    def go(src, dst, send, recv, where, keep=True):
        copy = remote(src, dst, send, recv, where)
        copy.start()
        if keep:
            pending.append(copy)
        return copy

    def arrived(dst, send, recv):
        remote(dst, dst, send, recv, partner).wait_recv()

    def owner_rows(dt, dp):
        return pl.ds(pl.multiple_of(place_at(dt, dp) * depth, 8), depth)

    def rows_of(index, size=128):
        return pl.ds(pl.multiple_of(index * size, size), size)

    own_thin = wall.at[r, pl.ds(pl.multiple_of(c * thin, 8), thin)]
    locals_ = [
        pltpu.make_async_copy(block_hbm, own_thin, local_sem.at[0]),
        pltpu.make_async_copy(panel_hbm, pbuf.at[0, pl.ds(0, depth)], local_sem.at[1]),
        pltpu.make_async_copy(rhs_hbm, rhs, local_sem.at[2]),
    ] + [
        pltpu.make_async_copy(tail_hbm.at[owner_rows(0, d)], tbuf.at[0, PLACE[d], pl.ds(0, depth)], local_sem.at[3 + d])
        for d in range(SIDE)
    ]
    for copy in locals_:
        copy.start()

    barrier = pltpu.get_barrier_semaphore()
    greeted = [at_x(p1), at_x(p2), partner] + [
        {"row": 2 * x + core, "col": place_at(*offset)}
        for core in range(2) for d in (1, 2, 3) for offset in ((d, 0), (0, d))
    ]
    for where in greeted:
        pl.semaphore_signal(barrier, inc=1, device_id=where, device_id_type=MESH)
    pl.semaphore_wait(barrier, len(greeted))

    def part_rows(i):
        return pl.ds(sum(CUTS[:i]) * unit, CUTS[i] * unit)

    def send_panel(i):
        go(panel_hbm.at[part_rows(i)], pbuf.at[2, part_rows(i)], p_s.at[0, i], p_r.at[2, i], at_p(1))
        go(panel_hbm.at[part_rows(i)], pbuf.at[1, part_rows(i)], p_s.at[1, i], p_r.at[1, i], at_p(3))

    for d in (2, 1, 3):
        go(block_hbm, own_thin, wz_s.at[d], wz_r.at[SIDE - d], at_t(d))
    send_panel(0)

    def clear(i, _):
        inv[rows_of(i), :] = jnp.zeros((128, window), F32)
        return 0

    lax.fori_loop(0, window // 128, clear, 0)
    zeros = jnp.zeros((pad - depth, width), F32)
    for j in range(SIDE):
        for q in range(SIDE):
            tbuf[j, q, pl.ds(depth, pad - depth), :] = zeros
    for q in range(SIDE):
        pbuf[q, pl.ds(depth, pad - depth), :] = jnp.zeros((pad - depth, window), F32)

    def thin_rows(dt, dp):
        return wall.at[r, pl.ds(pl.multiple_of(place_at(dt, dp) * thin, 8), thin)]

    locals_[0].wait()
    for d in (1, 3, 2):
        arrived(thin_rows(d, 0), wz_s.at[d], wz_r.at[d])
    thin_copies = []
    pc = k * z + (1 - k) * y
    near = 1 - 2 * (pc % 2)

    def swap_thin(sem, mine, where):
        for d in range(SIDE):
            thin_copies.append(
                go(thin_rows(d, mine), thin_rows(d, mine), wy_s.at[sem, d], wy_r.at[sem, d], at_p(where), False)
            )

    def thin_here(sem, theirs):
        for d in range(SIDE):
            arrived(thin_rows(d, theirs), wy_s.at[sem, d], wy_r.at[sem, d])

    swap_thin(0, 0, near)
    send_panel(1)
    thin_here(0, near)
    swap_thin(1, 0, -near)
    swap_thin(2, near, -near)
    for i in range(2, PARTS):
        send_panel(i)
    thin_here(1, -near)
    thin_here(2, 2)
    for copy in thin_copies:
        copy.wait_send()

    diag = rows_of(r, share)
    wall[r, :, diag] = lower_inverse(wall[r, :, diag])
    def came_from(i):
        return 2 if i < FORTH else 1

    def pass_panel(i):
        side = came_from(i)
        arrived(pbuf.at[side, part_rows(i)], p_s.at[2, i], p_r.at[side, i])
        go(pbuf.at[side, part_rows(i)], pbuf.at[3, part_rows(i)], p_s.at[2, i], p_r.at[3, i], at_p(2 * side - 3))

    def strip_to_core(i, other):
        go(wall.at[2 * other + k], wall.at[2 * other + k], wc_s.at[i], wc_r.at[i], partner)

    go(wall.at[r], wall.at[r], wa_s, wa_r, at_x(p2))
    go(wall.at[r], wall.at[r], wb_s.at[0], wb_r.at[0], at_x(p1))
    strip_to_core(0, x)
    for i in range(FORTH):
        pass_panel(i)
    arrived(wall.at[2 * p2 + k], wa_s, wa_r)
    go(wall.at[2 * p2 + k], wall.at[2 * p2 + k], wb_s.at[1], wb_r.at[1], at_x(p1))
    strip_to_core(1, p2)
    for i in range(FORTH, PARTS):
        pass_panel(i)

    for q in (0, 1, 3, 2):
        for d in (1, 3):
            go(tail_hbm.at[owner_rows(d, q)], tbuf.at[SIDE - d, PLACE[q], pl.ds(0, depth)],
               t_s.at[d, PLACE[q]], t_r.at[SIDE - d, PLACE[q]], at_t(d))
    for h in range(2):
        for q in (0, 1, 3, 2):
            go(tail_hbm.at[owner_rows(2, q), pl.ds(h * lane, lane)], relay.at[h, PLACE[q]],
               r_s.at[h, PLACE[q]], r_r.at[h, PLACE[q]], at_t(1 + 2 * (PLACE[q] % 2)))

    arrived(wall.at[2 * p1 + k], wb_s.at[0], wb_r.at[0])
    strip_to_core(2, p1)
    arrived(wall.at[2 * p12 + k], wb_s.at[1], wb_r.at[1])
    strip_to_core(3, p12)

    for i, other in enumerate((x, p1, p2, p12)):
        arrived(wall.at[2 * other + 1 - k], wc_s.at[i], wc_r.at[i])

    blocks = window // share
    for i in range(blocks):
        inv[pl.ds(i * share, share), pl.ds(i * share, share)] = wall[i, :, pl.ds(i * share, share)]
    size = share
    while size < window:
        count = size // share
        strip = min(size, 256)
        for base in range(0, window, 2 * size):
            top, low_rows = pl.ds(base, size), pl.ds(base + size, size)

            def below(i, _, base=base, size=size, count=count, strip=strip, top=top, low_rows=low_rows):
                start = pl.multiple_of(i * strip, strip)
                left = inv[pl.ds(base + size + start, strip), low_rows]
                under = wall[pl.ds(base // share + count, count), :, top].reshape(size, size)
                tmp[pl.ds(0, strip), pl.ds(0, size)] = dot(left, under)
                inv[pl.ds(base + size + start, strip), top] = -dot(tmp[pl.ds(0, strip), pl.ds(0, size)], inv[top, top])
                return 0

            if strip == size:
                below(0, 0)
            else:
                lax.fori_loop(0, size // strip, below, 0)
        size *= 2

    def split_inverse(i, _):
        high, rest = halves(inv[rows_of(i), :])
        inv_hi[rows_of(i), :] = high
        inv_lo[rows_of(i), :] = rest
        return 0

    lax.fori_loop(0, window // 128, split_inverse, 0)

    def pass_tail(h):
        for q in range(SIDE):
            arrived(relay.at[h, q], r_s.at[h, q], r_r.at[h, q])
            go(relay.at[h, q], tbuf.at[2, q, pl.ds(0, depth), pl.ds(h * lane, lane)],
               f_s.at[h, q], f_r.at[h, q], at_t(1 + 2 * (q % 2)))

    def turn_panel(q, _):
        def split_rows(i, _):
            high, rest = halves(pbuf[q, rows_of(i), :])
            phi[rows_of(i), :] = high
            plo[rows_of(i), :] = rest
            return 0

        lax.fori_loop(0, pad // 128, split_rows, 0)
        place = pl.ds(pl.multiple_of(q * pad, pad), pad)
        for n in range(0, window, 256):
            deep, cols = pl.ds(n, window - n), pl.ds(n, 256)
            product = (
                mm(phi[:, deep], inv_hi[deep, cols])
                + mm(phi[:, deep], inv_lo[deep, cols])
                + mm(plo[:, deep], inv_hi[deep, cols])
            )
            high, rest = halves(-product.T)
            pthi[cols, place] = high
            ptlo[cols, place] = rest
        return 0

    def panel_here(q):
        for i in range(PARTS):
            if q != came_from(i):
                arrived(pbuf.at[q, part_rows(i)], p_s.at[0, i], p_r.at[q, i])

    locals_[1].wait()
    panel_here(1)
    panel_here(2)
    lax.fori_loop(0, 3, turn_panel, 0)

    def take_tail(j, places, cols):
        for q in places:
            high, rest = halves(tbuf[j, q, :, cols])
            thi[pl.ds(q * pad, pad), cols] = high
            tlo[pl.ds(q * pad, pad), cols] = rest

    strip = 512

    def product(j, places, cols, fresh):
        take_tail(j, places, cols)
        deep = pl.ds(places[0] * pad, len(places) * pad)

        def one(i, _):
            rows = rows_of(i, strip)
            total = (
                mm(pthi[rows, deep], thi[deep, cols])
                + mm(pthi[rows, deep], tlo[deep, cols])
                + mm(ptlo[rows, deep], thi[deep, cols])
            )
            for h in range(total.shape[1] // lane):
                u = 2 * j + h + cols.start // lane
                piece = total[:, h * lane:(h + 1) * lane]
                sums[u, rows, :] = piece if fresh else sums[u, rows, :] + piece
            return 0

        lax.fori_loop(0, window // strip, one, 0)

    whole = pl.ds(0, width)
    def beside(j, places, fresh):
        for q in places:
            arrived(tbuf.at[j, q, pl.ds(0, depth)], t_s.at[1, q], t_r.at[j, q])
        product(j, places, whole, fresh)

    def cross(h, places, fresh):
        for q in places:
            arrived(tbuf.at[2, q, pl.ds(0, depth), pl.ds(h * lane, lane)], f_s.at[h, q], f_r.at[h, q])
        product(2, places, pl.ds(h * lane, lane), fresh)

    def lines(u, xx):
        return rows_of(xx, 2 * share) if u > 1 else rows_of(2 * xx + k, share)

    def height(u):
        return pl.ds(0, 2 * share if u > 1 else share)

    def to_core(u):
        for i in range(SIDE):
            go(sums.at[u, rows_of(2 * i + 1 - k, share)], core_in.at[u, i], c_s.at[u, i], c_r.at[u, i], partner)

    def to_first(u):
        if u < 2:
            for i in range(SIDE):
                arrived(core_in.at[u, i], c_s.at[u, i], c_r.at[u, i])
                rows = rows_of(2 * i + k, share)
                sums[u, rows, :] = sums[u, rows, :] + core_in[u, i]
        for i, other in ((1, p12), (0, p1)):
            go(sums.at[u, lines(u, other)], first_in.at[u, i, height(u)], a_s.at[u, i], a_r.at[u, i], at_x(p1))

    def to_second(u):
        for i, other in ((1, p2), (0, x)):
            arrived(first_in.at[u, i, height(u)], a_s.at[u, i], a_r.at[u, i])
            rows = lines(u, other)
            sums[u, rows, :] = sums[u, rows, :] + first_in[u, i, height(u), :]
            if i == 1:
                go(sums.at[u, rows], second_in.at[u, height(u)], b_s.at[u], b_r.at[u], at_x(p2))

    def to_last(u):
        j, h = u // 2, u % 2
        arrived(second_in.at[u, height(u)], b_s.at[u], b_r.at[u])
        rows = lines(u, x)
        sums[u, rows, :] = sums[u, rows, :] + second_in[u, height(u), :]
        if j:
            for i, core in enumerate((k, 1 - k)):
                go(sums.at[u, rows_of(2 * x + core, share)], last_in.at[k, SIDE - j, h],
                   l_s.at[i, u], l_r.at[k, SIDE - j, h], {"row": 2 * x + core, "col": place_at(j, 0)})

    def both(stage, j):
        stage(2 * j)
        stage(2 * j + 1)

    for copy in locals_[2:]:
        copy.wait()
    product(0, (0, 1, 2), whole, True)
    rhs_hi, rhs_lo = halves(rhs[...])
    own_hi, own_lo = inv_hi[rows_of(r, share), :], inv_lo[rows_of(r, share), :]
    own = mm_t(own_hi, rhs_hi) + mm_t(own_hi, rhs_lo) + mm_t(own_lo, rhs_hi)
    for h in range(2):
        sums[h] = sums[h] + own[:, h * lane:(h + 1) * lane]
    panel_here(3)
    turn_panel(3, 0)
    product(0, (3,), whole, False)
    both(to_core, 0)
    beside(1, (0, 1), True)
    both(to_first, 0)
    beside(3, (0, 1), True)
    beside(1, (2, 3), False)
    both(to_first, 1)
    beside(3, (2, 3), False)
    both(to_first, 3)
    both(to_second, 0)
    pass_tail(0)
    pass_tail(1)
    both(to_last, 0)
    both(to_second, 1)
    cross(0, (0, 1), True)
    cross(0, (2, 3), False)
    to_first(4)
    both(to_last, 1)
    cross(1, (0, 1), True)
    both(to_second, 3)
    cross(1, (2, 3), False)
    to_first(5)
    to_second(4)
    both(to_last, 3)
    to_second(5)
    to_last(4)
    to_last(5)

    rows = rows_of(r, share)
    for h in range(2):
        total = sums[h, rows, :]
        for core, d in ((k, 1), (1 - k, 1), (k, 3), (1 - k, 3), (k, 2), (1 - k, 2)):
            arrived(last_in.at[core, d, h], l_s.at[0, 0], l_r.at[core, d, h])
            total = total + last_in[core, d, h]
        out_ref[:, h * lane:(h + 1) * lane] = total

    for copy in pending:
        copy.wait_send()


def per_device(tail_vectors, lower_panel, window_rhs, window_block):
    columns = tail_vectors.shape[1]
    depth, window = lower_panel.shape
    share = window_rhs.shape[0]
    lane = columns // 2
    pad = -(-depth // 128) * 128
    groups = window // share
    dma = pltpu.SemaphoreType.DMA
    anywhere = pl.BlockSpec(memory_space=pl.ANY)
    return pl.pallas_call(
        kernel,
        out_shape=jax.ShapeDtypeStruct((share, columns), F32),
        in_specs=[anywhere] * 4,
        out_specs=pl.BlockSpec(memory_space=pltpu.VMEM),
        scratch_shapes=[
            pltpu.VMEM((SIDE, SIDE, pad, columns), F32),
            pltpu.VMEM((2, SIDE, depth, lane), F32),
            pltpu.VMEM((SIDE, pad, window), F32),
            pltpu.VMEM((pad, window), BF16),
            pltpu.VMEM((pad, window), BF16),
            pltpu.VMEM((window, SIDE * pad), BF16),
            pltpu.VMEM((window, SIDE * pad), BF16),
            pltpu.VMEM((groups, share, window), F32),
            pltpu.VMEM((window, window), F32),
            pltpu.VMEM((window, window), BF16),
            pltpu.VMEM((window, window), BF16),
            pltpu.VMEM((256, window // 2), F32),
            pltpu.VMEM((share, columns), F32),
            pltpu.VMEM((SIDE * pad, columns), BF16),
            pltpu.VMEM((SIDE * pad, columns), BF16),
            pltpu.VMEM((2 * SIDE, window, lane), F32),
            pltpu.VMEM((2, SIDE, share, lane), F32),
            pltpu.VMEM((2 * SIDE, 2, 2 * share, lane), F32),
            pltpu.VMEM((2 * SIDE, 2 * share, lane), F32),
            pltpu.VMEM((2, SIDE, 2, share, lane), F32),
            dma((7,)),
            dma((SIDE,)), dma((SIDE,)), dma((3, SIDE)), dma((3, SIDE)),
            dma, dma, dma((2,)), dma((2,)), dma((SIDE,)), dma((SIDE,)),
            dma((3, PARTS)), dma((SIDE, PARTS)),
            dma((SIDE, SIDE)), dma((SIDE, SIDE)),
            dma((2, SIDE)), dma((2, SIDE)), dma((2, SIDE)), dma((2, SIDE)),
            dma((2, SIDE)), dma((2, SIDE)),
            dma((2 * SIDE, 2)), dma((2 * SIDE, 2)),
            dma((2 * SIDE,)), dma((2 * SIDE,)),
            dma((2, 2 * SIDE)), dma((2, SIDE, 2)),
        ],
        compiler_params=pltpu.CompilerParams(
            collective_id=0, has_side_effects=True, vmem_limit_bytes=65000 * 1024
        ),
    )(tail_vectors, lower_panel, window_block, window_rhs)


def solution(mesh):
    in_specs = (P("row", "col"), P(("row", "col"), None), P("row", "col"), P(("row", "col"), None))
    out_specs = P("row", "col")
    return jax.shard_map(per_device, mesh=mesh, in_specs=in_specs, out_specs=out_specs, check_vma=False)
```

```python
import functools

import jax
import jax.numpy as jnp
from jax import lax
from jax.experimental import pallas as pl
from jax.experimental.pallas import tpu as pltpu
from jax.sharding import PartitionSpec as P

MESH = pl.DeviceIdType.MESH
HIGHEST = lax.Precision.HIGHEST
F32 = jnp.float32
BF16 = jnp.bfloat16
SIDE = 4
PLACE = (0, 1, 3, 2)
CUTS = (13, 8, 7, 5, 10, 10, 10)
PARTS = len(CUTS)
FORTH = 4


def dot(a, b):
    return jnp.dot(a, b, precision=HIGHEST, preferred_element_type=F32)


def mm_t(a, b):
    return lax.dot_general(a, b, (((0,), (0,)), ((), ())), preferred_element_type=F32)


def mm(a, b):
    return jnp.dot(a, b, preferred_element_type=F32)


def halves(a):
    high = a.astype(BF16)
    return high, (a - high.astype(F32)).astype(BF16)


def dot_split(a, b):
    a_hi, a_lo = halves(a)
    b_hi, b_lo = halves(b)
    return mm(a_hi, b_hi) + mm(a_hi, b_lo) + mm(a_lo, b_hi)


def lower_inverse(block, base=32):
    size = block.shape[0]
    rows = lax.broadcasted_iota(jnp.int32, (size, size), 0)
    cols = lax.broadcasted_iota(jnp.int32, (size, size), 1)
    eye = jnp.where(rows == cols, 1.0, 0.0)
    diag_col = jnp.sum(jnp.where(rows == cols, block, 0.0), axis=1, keepdims=True)
    diag_row = jnp.sum(jnp.where(rows == cols, block, 0.0), axis=0, keepdims=True)
    near = (rows // base == cols // base) & (rows > cols)
    power = jnp.where(near, -block / diag_col, 0.0)
    inverse = eye + power
    reach = 2
    while reach < base:
        power = dot(power, power)
        inverse = inverse + dot(inverse, power)
        reach *= 2
    inverse = inverse / diag_row
    while base < size:
        below = (rows // (2 * base) == cols // (2 * base)) & (rows // base > cols // base)
        inverse = inverse - dot(dot(inverse, jnp.where(below, block, 0.0)), inverse)
        base *= 2
    return inverse


def kernel(
    tail_hbm, panel_hbm, block_hbm, rhs_hbm, out_ref,
    tbuf, relay, pbuf, phi, plo, pthi, ptlo, wall, inv, inv_hi, inv_lo, tmp, rhs, thi, tlo,
    sums, core_in, first_in, second_in, last_in,
    local_sem, wz_s, wz_r, wy_s, wy_r, wa_s, wa_r, wb_s, wb_r, wc_s, wc_r,
    p_s, p_r, t_s, t_r, r_s, r_r, f_s, f_r,
    c_s, c_r, a_s, a_r, b_s, b_r, l_s, l_r,
):
    depth, window = panel_hbm.shape
    thin = block_hbm.shape[0]
    share, width = rhs_hbm.shape
    lane = width // 2
    pad = pbuf.shape[1]
    unit = depth // sum(CUTS)
    r = lax.axis_index("row")
    c = lax.axis_index("col")
    x, k = r // 2, r % 2
    z, y = c // SIDE, c % SIDE
    low, mirror = x + 1 - 2 * (x % 2), SIDE - 1 - x
    p1 = k * mirror + (1 - k) * low
    p2 = k * low + (1 - k) * mirror
    p12 = (x + 2) % SIDE

    def place_at(dt, dp):
        zz = (z + dt * (1 - k) + dp * k + 2 * SIDE) % SIDE
        yy = (y + dt * k + dp * (1 - k) + 2 * SIDE) % SIDE
        return zz * SIDE + yy

    def at_t(d):
        return {"row": r, "col": place_at(d, 0)}

    def at_p(d):
        return {"row": r, "col": place_at(0, d)}

    def at_x(other):
        return {"row": 2 * other + k, "col": c}

    partner = {"row": 2 * x + 1 - k, "col": c}
    pending = []

    def remote(src, dst, send, recv, where):
        return pltpu.make_async_remote_copy(
            src_ref=src, dst_ref=dst, send_sem=send, recv_sem=recv, device_id=where, device_id_type=MESH
        )

    def go(src, dst, send, recv, where, keep=True):
        copy = remote(src, dst, send, recv, where)
        copy.start()
        if keep:
            pending.append(copy)
        return copy

    def arrived(dst, send, recv):
        remote(dst, dst, send, recv, partner).wait_recv()

    def owner_rows(dt, dp):
        return pl.ds(pl.multiple_of(place_at(dt, dp) * depth, 8), depth)

    def rows_of(index, size=128):
        return pl.ds(pl.multiple_of(index * size, size), size)

    own_thin = wall.at[r, pl.ds(pl.multiple_of(c * thin, 8), thin)]
    locals_ = [
        pltpu.make_async_copy(block_hbm, own_thin, local_sem.at[0]),
        pltpu.make_async_copy(panel_hbm, pbuf.at[0, pl.ds(0, depth)], local_sem.at[1]),
        pltpu.make_async_copy(rhs_hbm, rhs, local_sem.at[2]),
    ] + [
        pltpu.make_async_copy(tail_hbm.at[owner_rows(0, d)], tbuf.at[0, PLACE[d], pl.ds(0, depth)], local_sem.at[3 + d])
        for d in range(SIDE)
    ]
    for copy in locals_:
        copy.start()

    barrier = pltpu.get_barrier_semaphore()
    greeted = [at_x(p1), at_x(p2), partner] + [
        {"row": 2 * x + core, "col": place_at(*offset)}
        for core in range(2) for d in (1, 2, 3) for offset in ((d, 0), (0, d))
    ]
    for where in greeted:
        pl.semaphore_signal(barrier, inc=1, device_id=where, device_id_type=MESH)
    pl.semaphore_wait(barrier, len(greeted))

    def part_rows(i):
        return pl.ds(sum(CUTS[:i]) * unit, CUTS[i] * unit)

    def send_panel(i):
        go(panel_hbm.at[part_rows(i)], pbuf.at[2, part_rows(i)], p_s.at[0, i], p_r.at[2, i], at_p(1))
        go(panel_hbm.at[part_rows(i)], pbuf.at[1, part_rows(i)], p_s.at[1, i], p_r.at[1, i], at_p(3))

    for d in (2, 1, 3):
        go(block_hbm, own_thin, wz_s.at[d], wz_r.at[SIDE - d], at_t(d))
    send_panel(0)

    def clear(i, _):
        inv[rows_of(i), :] = jnp.zeros((128, window), F32)
        return 0

    lax.fori_loop(0, window // 128, clear, 0)
    zeros = jnp.zeros((pad - depth, width), F32)
    for j in range(SIDE):
        for q in range(SIDE):
            tbuf[j, q, pl.ds(depth, pad - depth), :] = zeros
    for q in range(SIDE):
        pbuf[q, pl.ds(depth, pad - depth), :] = jnp.zeros((pad - depth, window), F32)

    def thin_rows(dt, dp):
        return wall.at[r, pl.ds(pl.multiple_of(place_at(dt, dp) * thin, 8), thin)]

    locals_[0].wait()
    for d in (1, 3, 2):
        arrived(thin_rows(d, 0), wz_s.at[d], wz_r.at[d])
    thin_copies = []
    pc = k * z + (1 - k) * y
    near = 1 - 2 * (pc % 2)

    def swap_thin(sem, mine, where):
        for d in range(SIDE):
            side = 1 if d < 2 else -1
            rows = thin_rows(d, side * mine)
            thin_copies.append(go(rows, rows, wy_s.at[sem, d], wy_r.at[sem, d], at_p(side * where), False))

    def thin_here(sem, theirs):
        for d in range(SIDE):
            arrived(thin_rows(d, theirs if d < 2 else -theirs), wy_s.at[sem, d], wy_r.at[sem, d])

    swap_thin(0, 0, near)
    send_panel(1)
    thin_here(0, near)
    swap_thin(1, 0, -near)
    swap_thin(2, near, -near)
    for i in range(2, PARTS):
        send_panel(i)
    thin_here(1, -near)
    thin_here(2, 2)
    for copy in thin_copies:
        copy.wait_send()

    diag = rows_of(r, share)
    wall[r, :, diag] = lower_inverse(wall[r, :, diag])
    def came_from(i):
        return 2 if i < FORTH else 1

    def pass_panel(i):
        side = came_from(i)
        arrived(pbuf.at[side, part_rows(i)], p_s.at[2, i], p_r.at[side, i])
        go(pbuf.at[side, part_rows(i)], pbuf.at[3, part_rows(i)], p_s.at[2, i], p_r.at[3, i], at_p(2 * side - 3))

    def strip_to_core(i, other):
        go(wall.at[2 * other + k], wall.at[2 * other + k], wc_s.at[i], wc_r.at[i], partner)

    go(wall.at[r], wall.at[r], wa_s, wa_r, at_x(p2))
    go(wall.at[r], wall.at[r], wb_s.at[0], wb_r.at[0], at_x(p1))
    strip_to_core(0, x)
    for i in range(PARTS - 1):
        pass_panel(i)
    arrived(wall.at[2 * p2 + k], wa_s, wa_r)
    go(wall.at[2 * p2 + k], wall.at[2 * p2 + k], wb_s.at[1], wb_r.at[1], at_x(p1))
    strip_to_core(1, p2)
    pass_panel(PARTS - 1)

    for q in (0, 1, 3, 2):
        for d in (1, 3):
            go(tail_hbm.at[owner_rows(d, q)], tbuf.at[SIDE - d, PLACE[q], pl.ds(0, depth)],
               t_s.at[d, PLACE[q]], t_r.at[SIDE - d, PLACE[q]], at_t(d))
    for h in range(2):
        for q in (0, 1, 3, 2):
            go(tail_hbm.at[owner_rows(2, q), pl.ds(h * lane, lane)], relay.at[h, PLACE[q]],
               r_s.at[h, PLACE[q]], r_r.at[h, PLACE[q]], at_t(1 + 2 * (PLACE[q] % 2)))

    arrived(wall.at[2 * p1 + k], wb_s.at[0], wb_r.at[0])
    strip_to_core(2, p1)
    arrived(wall.at[2 * p12 + k], wb_s.at[1], wb_r.at[1])
    strip_to_core(3, p12)

    for i, other in enumerate((x, p1, p2, p12)):
        arrived(wall.at[2 * other + 1 - k], wc_s.at[i], wc_r.at[i])

    blocks = window // share
    for i in range(blocks):
        inv[pl.ds(i * share, share), pl.ds(i * share, share)] = wall[i, :, pl.ds(i * share, share)]
    size = share
    while size < window:
        count = size // share
        strip = min(size, 256)
        for base in range(0, window, 2 * size):
            top, low_rows = pl.ds(base, size), pl.ds(base + size, size)

            def below(i, _, base=base, size=size, count=count, strip=strip, top=top, low_rows=low_rows):
                start = pl.multiple_of(i * strip, strip)
                left = inv[pl.ds(base + size + start, strip), low_rows]
                under = wall[pl.ds(base // share + count, count), :, top].reshape(size, size)
                times = dot if size == share else dot_split
                tmp[pl.ds(0, strip), pl.ds(0, size)] = times(left, under)
                inv[pl.ds(base + size + start, strip), top] = -times(tmp[pl.ds(0, strip), pl.ds(0, size)], inv[top, top])
                return 0

            if strip == size:
                below(0, 0)
            else:
                lax.fori_loop(0, size // strip, below, 0)
        size *= 2

    def split_inverse(i, _):
        high, rest = halves(inv[rows_of(i), :])
        inv_hi[rows_of(i), :] = high
        inv_lo[rows_of(i), :] = rest
        return 0

    lax.fori_loop(0, window // 128, split_inverse, 0)

    def pass_tail(h):
        for q in range(SIDE):
            arrived(relay.at[h, q], r_s.at[h, q], r_r.at[h, q])
            go(relay.at[h, q], tbuf.at[2, q, pl.ds(0, depth), pl.ds(h * lane, lane)],
               f_s.at[h, q], f_r.at[h, q], at_t(1 + 2 * (q % 2)))

    def turn_panel(q, _):
        def split_rows(i, _):
            high, rest = halves(pbuf[q, rows_of(i), :])
            phi[rows_of(i), :] = high
            plo[rows_of(i), :] = rest
            return 0

        lax.fori_loop(0, pad // 128, split_rows, 0)
        place = pl.ds(pl.multiple_of(q * pad, pad), pad)
        for n in range(0, window, 256):
            deep, cols = pl.ds(n, window - n), pl.ds(n, 256)
            product = (
                mm(phi[:, deep], inv_hi[deep, cols])
                + mm(phi[:, deep], inv_lo[deep, cols])
                + mm(plo[:, deep], inv_hi[deep, cols])
            )
            high, rest = halves(-product.T)
            pthi[cols, place] = high
            ptlo[cols, place] = rest
        return 0

    def panel_here(q):
        for i in range(PARTS):
            if q != came_from(i):
                arrived(pbuf.at[q, part_rows(i)], p_s.at[0, i], p_r.at[q, i])

    locals_[1].wait()
    panel_here(1)
    panel_here(2)
    lax.fori_loop(0, 3, turn_panel, 0)

    def take_tail(j, places, cols):
        for q in places:
            high, rest = halves(tbuf[j, q, :, cols])
            thi[pl.ds(q * pad, pad), cols] = high
            tlo[pl.ds(q * pad, pad), cols] = rest

    strip = 512

    def product(j, places, cols, fresh):
        take_tail(j, places, cols)
        deep = pl.ds(places[0] * pad, len(places) * pad)

        def one(i, _):
            rows = rows_of(i, strip)
            total = (
                mm(pthi[rows, deep], thi[deep, cols])
                + mm(pthi[rows, deep], tlo[deep, cols])
                + mm(ptlo[rows, deep], thi[deep, cols])
            )
            for h in range(total.shape[1] // lane):
                u = 2 * j + h + cols.start // lane
                piece = total[:, h * lane:(h + 1) * lane]
                sums[u, rows, :] = piece if fresh else sums[u, rows, :] + piece
            return 0

        lax.fori_loop(0, window // strip, one, 0)

    whole = pl.ds(0, width)
    def beside(j, places, fresh):
        for q in places:
            arrived(tbuf.at[j, q, pl.ds(0, depth)], t_s.at[1, q], t_r.at[j, q])
        product(j, places, whole, fresh)

    def cross(h, places, fresh):
        for q in places:
            arrived(tbuf.at[2, q, pl.ds(0, depth), pl.ds(h * lane, lane)], f_s.at[h, q], f_r.at[h, q])
        product(2, places, pl.ds(h * lane, lane), fresh)

    def lines(u, xx):
        return rows_of(xx, 2 * share) if u > 1 else rows_of(2 * xx + k, share)

    def height(u):
        return pl.ds(0, 2 * share if u > 1 else share)

    def to_core(u):
        for i in range(SIDE):
            go(sums.at[u, rows_of(2 * i + 1 - k, share)], core_in.at[u, i], c_s.at[u, i], c_r.at[u, i], partner)

    def to_first(u):
        if u < 2:
            for i in range(SIDE):
                arrived(core_in.at[u, i], c_s.at[u, i], c_r.at[u, i])
                rows = rows_of(2 * i + k, share)
                sums[u, rows, :] = sums[u, rows, :] + core_in[u, i]
        for i, other in ((1, p12), (0, p1)):
            go(sums.at[u, lines(u, other)], first_in.at[u, i, height(u)], a_s.at[u, i], a_r.at[u, i], at_x(p1))

    def to_second(u):
        for i, other in ((1, p2), (0, x)):
            arrived(first_in.at[u, i, height(u)], a_s.at[u, i], a_r.at[u, i])
            rows = lines(u, other)
            sums[u, rows, :] = sums[u, rows, :] + first_in[u, i, height(u), :]
            if i == 1:
                go(sums.at[u, rows], second_in.at[u, height(u)], b_s.at[u], b_r.at[u], at_x(p2))

    def to_last(u):
        j, h = u // 2, u % 2
        arrived(second_in.at[u, height(u)], b_s.at[u], b_r.at[u])
        rows = lines(u, x)
        sums[u, rows, :] = sums[u, rows, :] + second_in[u, height(u), :]
        if j:
            for i, core in enumerate((k, 1 - k)):
                go(sums.at[u, rows_of(2 * x + core, share)], last_in.at[k, SIDE - j, h],
                   l_s.at[i, u], l_r.at[k, SIDE - j, h], {"row": 2 * x + core, "col": place_at(j, 0)})

    def both(stage, j):
        stage(2 * j)
        stage(2 * j + 1)

    for copy in locals_[2:]:
        copy.wait()
    product(0, (0, 1, 2), whole, True)
    rhs_hi, rhs_lo = halves(rhs[...])
    own_hi, own_lo = inv_hi[rows_of(r, share), :], inv_lo[rows_of(r, share), :]
    own = mm_t(own_hi, rhs_hi) + mm_t(own_hi, rhs_lo) + mm_t(own_lo, rhs_hi)
    for h in range(2):
        sums[h] = sums[h] + own[:, h * lane:(h + 1) * lane]
    panel_here(3)
    turn_panel(3, 0)
    product(0, (3,), whole, False)
    both(to_core, 0)
    beside(1, (0,), True)
    both(to_first, 0)
    beside(1, (1, 2, 3), False)
    both(to_first, 1)
    beside(3, (0, 1, 2, 3), True)
    both(to_first, 3)
    both(to_second, 0)
    pass_tail(0)
    pass_tail(1)
    both(to_last, 0)
    both(to_second, 1)
    cross(0, (0, 1), True)
    cross(0, (2, 3), False)
    to_first(4)
    both(to_second, 3)
    both(to_last, 1)
    cross(1, (0, 1), True)
    cross(1, (2, 3), False)
    to_first(5)
    to_second(4)
    both(to_last, 3)
    to_second(5)
    to_last(4)
    to_last(5)

    rows = rows_of(r, share)
    for h in range(2):
        total = sums[h, rows, :]
        for core, d in ((k, 1), (1 - k, 1), (k, 3), (1 - k, 3), (k, 2), (1 - k, 2)):
            arrived(last_in.at[core, d, h], l_s.at[0, 0], l_r.at[core, d, h])
            total = total + last_in[core, d, h]
        out_ref[:, h * lane:(h + 1) * lane] = total

    for copy in pending:
        copy.wait_send()


def per_device(tail_vectors, lower_panel, window_rhs, window_block):
    columns = tail_vectors.shape[1]
    depth, window = lower_panel.shape
    share = window_rhs.shape[0]
    lane = columns // 2
    pad = -(-depth // 128) * 128
    groups = window // share
    dma = pltpu.SemaphoreType.DMA
    anywhere = pl.BlockSpec(memory_space=pl.ANY)
    return pl.pallas_call(
        kernel,
        out_shape=pltpu.VMEM((share, columns), F32),
        in_specs=[anywhere] * 4,
        out_specs=pl.BlockSpec(memory_space=pltpu.VMEM),
        scratch_shapes=[
            pltpu.VMEM((SIDE, SIDE, pad, columns), F32),
            pltpu.VMEM((2, SIDE, depth, lane), F32),
            pltpu.VMEM((SIDE, pad, window), F32),
            pltpu.VMEM((pad, window), BF16),
            pltpu.VMEM((pad, window), BF16),
            pltpu.VMEM((window, SIDE * pad), BF16),
            pltpu.VMEM((window, SIDE * pad), BF16),
            pltpu.VMEM((groups, share, window), F32),
            pltpu.VMEM((window, window), F32),
            pltpu.VMEM((window, window), BF16),
            pltpu.VMEM((window, window), BF16),
            pltpu.VMEM((256, window // 2), F32),
            pltpu.VMEM((share, columns), F32),
            pltpu.VMEM((SIDE * pad, columns), BF16),
            pltpu.VMEM((SIDE * pad, columns), BF16),
            pltpu.VMEM((2 * SIDE, window, lane), F32),
            pltpu.VMEM((2, SIDE, share, lane), F32),
            pltpu.VMEM((2 * SIDE, 2, 2 * share, lane), F32),
            pltpu.VMEM((2 * SIDE, 2 * share, lane), F32),
            pltpu.VMEM((2, SIDE, 2, share, lane), F32),
            dma((7,)),
            dma((SIDE,)), dma((SIDE,)), dma((3, SIDE)), dma((3, SIDE)),
            dma, dma, dma((2,)), dma((2,)), dma((SIDE,)), dma((SIDE,)),
            dma((3, PARTS)), dma((SIDE, PARTS)),
            dma((SIDE, SIDE)), dma((SIDE, SIDE)),
            dma((2, SIDE)), dma((2, SIDE)), dma((2, SIDE)), dma((2, SIDE)),
            dma((2, SIDE)), dma((2, SIDE)),
            dma((2 * SIDE, 2)), dma((2 * SIDE, 2)),
            dma((2 * SIDE,)), dma((2 * SIDE,)),
            dma((2, 2 * SIDE)), dma((2, SIDE, 2)),
        ],
        compiler_params=pltpu.CompilerParams(
            collective_id=0, has_side_effects=True, vmem_limit_bytes=65000 * 1024
        ),
    )(tail_vectors, lower_panel, window_block, window_rhs)


def solution(mesh):
    in_specs = (P("row", "col"), P(("row", "col"), None), P("row", "col"), P(("row", "col"), None))
    out_specs = P("row", "col")
    return jax.shard_map(per_device, mesh=mesh, in_specs=in_specs, out_specs=out_specs, check_vma=False)
```

```python
import functools

import jax
import jax.numpy as jnp
from jax import lax
from jax.experimental import pallas as pl
from jax.experimental.pallas import tpu as pltpu
from jax.sharding import PartitionSpec as P

MESH = pl.DeviceIdType.MESH
HIGHEST = lax.Precision.HIGHEST
F32 = jnp.float32
BF16 = jnp.bfloat16
SIDE = 4
PLACE = (0, 1, 3, 2)
CUTS = (13, 8, 7, 5, 10, 10, 10)
PARTS = len(CUTS)
FORTH = 4


def dot(a, b):
    return jnp.dot(a, b, precision=HIGHEST, preferred_element_type=F32)


def mm_t(a, b):
    return lax.dot_general(a, b, (((0,), (0,)), ((), ())), preferred_element_type=F32)


def mm(a, b):
    return jnp.dot(a, b, preferred_element_type=F32)


def halves(a):
    high = a.astype(BF16)
    return high, (a - high.astype(F32)).astype(BF16)


def dot_split(a, b):
    a_hi, a_lo = halves(a)
    b_hi, b_lo = halves(b)
    return mm(a_hi, b_hi) + mm(a_hi, b_lo) + mm(a_lo, b_hi)


def lower_inverse(block, base=32):
    size = block.shape[0]
    rows = lax.broadcasted_iota(jnp.int32, (size, size), 0)
    cols = lax.broadcasted_iota(jnp.int32, (size, size), 1)
    eye = jnp.where(rows == cols, 1.0, 0.0)
    diag_col = jnp.sum(jnp.where(rows == cols, block, 0.0), axis=1, keepdims=True)
    diag_row = jnp.sum(jnp.where(rows == cols, block, 0.0), axis=0, keepdims=True)
    near = (rows // base == cols // base) & (rows > cols)
    power = jnp.where(near, -block / diag_col, 0.0)
    inverse = eye + power
    reach = 2
    while reach < base:
        power = dot(power, power)
        inverse = inverse + dot(inverse, power)
        reach *= 2
    inverse = inverse / diag_row
    while base < size:
        below = (rows // (2 * base) == cols // (2 * base)) & (rows // base > cols // base)
        inverse = inverse - dot(dot(inverse, jnp.where(below, block, 0.0)), inverse)
        base *= 2
    return inverse


def kernel(
    tail_hbm, panel_hbm, block_hbm, rhs_hbm, out_ref,
    tbuf, relay, pbuf, phi, plo, pthi, ptlo, wall, inv, inv_hi, inv_lo, tmp, rhs, thi, tlo,
    sums, core_in, first_in, second_in, last_in,
    local_sem, wz_s, wz_r, wy_s, wy_r, wa_s, wa_r, wb_s, wb_r, wc_s, wc_r,
    p_s, p_r, t_s, t_r, r_s, r_r, f_s, f_r,
    c_s, c_r, a_s, a_r, b_s, b_r, l_s, l_r,
):
    depth, window = panel_hbm.shape
    thin = block_hbm.shape[0]
    share, width = rhs_hbm.shape
    lane = width // 2
    pad = pbuf.shape[1]
    unit = depth // sum(CUTS)
    r = lax.axis_index("row")
    c = lax.axis_index("col")
    x, k = r // 2, r % 2
    z, y = c // SIDE, c % SIDE
    low, mirror = x + 1 - 2 * (x % 2), SIDE - 1 - x
    p1 = k * mirror + (1 - k) * low
    p2 = k * low + (1 - k) * mirror
    p12 = (x + 2) % SIDE

    def place_at(dt, dp):
        zz = (z + dt * (1 - k) + dp * k + 2 * SIDE) % SIDE
        yy = (y + dt * k + dp * (1 - k) + 2 * SIDE) % SIDE
        return zz * SIDE + yy

    def at_t(d):
        return {"row": r, "col": place_at(d, 0)}

    def at_p(d):
        return {"row": r, "col": place_at(0, d)}

    def at_x(other):
        return {"row": 2 * other + k, "col": c}

    partner = {"row": 2 * x + 1 - k, "col": c}
    pending = []

    def remote(src, dst, send, recv, where):
        return pltpu.make_async_remote_copy(
            src_ref=src, dst_ref=dst, send_sem=send, recv_sem=recv, device_id=where, device_id_type=MESH
        )

    def go(src, dst, send, recv, where, keep=True):
        copy = remote(src, dst, send, recv, where)
        copy.start()
        if keep:
            pending.append(copy)
        return copy

    def arrived(dst, send, recv):
        remote(dst, dst, send, recv, partner).wait_recv()

    def owner_rows(dt, dp):
        return pl.ds(pl.multiple_of(place_at(dt, dp) * depth, 8), depth)

    def rows_of(index, size=128):
        return pl.ds(pl.multiple_of(index * size, size), size)

    own_thin = wall.at[r, pl.ds(pl.multiple_of(c * thin, 8), thin)]
    locals_ = [
        pltpu.make_async_copy(block_hbm, own_thin, local_sem.at[0]),
        pltpu.make_async_copy(panel_hbm, pbuf.at[0, pl.ds(0, depth)], local_sem.at[1]),
        pltpu.make_async_copy(rhs_hbm, rhs, local_sem.at[2]),
    ] + [
        pltpu.make_async_copy(tail_hbm.at[owner_rows(0, d)], tbuf.at[0, PLACE[d], pl.ds(0, depth)], local_sem.at[3 + d])
        for d in range(SIDE)
    ]
    for copy in locals_:
        copy.start()

    barrier = pltpu.get_barrier_semaphore()
    greeted = [at_x(p1), at_x(p2), partner] + [
        {"row": 2 * x + core, "col": place_at(*offset)}
        for core in range(2) for d in (1, 2, 3) for offset in ((d, 0), (0, d))
    ]
    for where in greeted:
        pl.semaphore_signal(barrier, inc=1, device_id=where, device_id_type=MESH)
    pl.semaphore_wait(barrier, len(greeted))

    def part_rows(i):
        return pl.ds(sum(CUTS[:i]) * unit, CUTS[i] * unit)

    def send_panel(i):
        go(panel_hbm.at[part_rows(i)], pbuf.at[2, part_rows(i)], p_s.at[0, i], p_r.at[2, i], at_p(1))
        go(panel_hbm.at[part_rows(i)], pbuf.at[1, part_rows(i)], p_s.at[1, i], p_r.at[1, i], at_p(3))

    for d in (2, 1, 3):
        go(block_hbm, own_thin, wz_s.at[d], wz_r.at[SIDE - d], at_t(d))
    send_panel(0)

    def clear(i, _):
        inv[rows_of(i), :] = jnp.zeros((128, window), F32)
        return 0

    lax.fori_loop(0, window // 128, clear, 0)
    zeros = jnp.zeros((pad - depth, width), F32)
    for j in range(SIDE):
        for q in range(SIDE):
            tbuf[j, q, pl.ds(depth, pad - depth), :] = zeros
    for q in range(SIDE):
        pbuf[q, pl.ds(depth, pad - depth), :] = jnp.zeros((pad - depth, window), F32)

    def thin_rows(dt, dp):
        return wall.at[r, pl.ds(pl.multiple_of(place_at(dt, dp) * thin, 8), thin)]

    locals_[0].wait()
    for d in (1, 3, 2):
        arrived(thin_rows(d, 0), wz_s.at[d], wz_r.at[d])
    thin_copies = []
    pc = k * z + (1 - k) * y
    near = 1 - 2 * (pc % 2)

    def swap_thin(sem, mine, where):
        for d in range(SIDE):
            side = 1 if d < 2 else -1
            rows = thin_rows(d, side * mine)
            thin_copies.append(go(rows, rows, wy_s.at[sem, d], wy_r.at[sem, d], at_p(side * where), False))

    def thin_here(sem, theirs):
        for d in range(SIDE):
            arrived(thin_rows(d, theirs if d < 2 else -theirs), wy_s.at[sem, d], wy_r.at[sem, d])

    swap_thin(0, 0, near)
    send_panel(1)
    thin_here(0, near)
    swap_thin(1, 0, -near)
    swap_thin(2, near, -near)
    for i in range(2, PARTS):
        send_panel(i)
    thin_here(1, -near)
    thin_here(2, 2)
    for copy in thin_copies:
        copy.wait_send()

    diag = rows_of(r, share)
    wall[r, :, diag] = lower_inverse(wall[r, :, diag])
    def came_from(i):
        return 2 if i < FORTH else 1

    def pass_panel(i):
        side = came_from(i)
        arrived(pbuf.at[side, part_rows(i)], p_s.at[2, i], p_r.at[side, i])
        go(pbuf.at[side, part_rows(i)], pbuf.at[3, part_rows(i)], p_s.at[2, i], p_r.at[3, i], at_p(2 * side - 3))

    def strip_to_core(i, other):
        go(wall.at[2 * other + k], wall.at[2 * other + k], wc_s.at[i], wc_r.at[i], partner)

    go(wall.at[r], wall.at[r], wa_s, wa_r, at_x(p2))
    go(wall.at[r], wall.at[r], wb_s.at[0], wb_r.at[0], at_x(p1))
    strip_to_core(0, x)
    for i in range(PARTS - 1):
        pass_panel(i)
    arrived(wall.at[2 * p2 + k], wa_s, wa_r)
    go(wall.at[2 * p2 + k], wall.at[2 * p2 + k], wb_s.at[1], wb_r.at[1], at_x(p1))
    strip_to_core(1, p2)
    pass_panel(PARTS - 1)

    for q in (0, 1, 3, 2):
        for d in (1, 3):
            go(tail_hbm.at[owner_rows(d, q)], tbuf.at[SIDE - d, PLACE[q], pl.ds(0, depth)],
               t_s.at[d, PLACE[q]], t_r.at[SIDE - d, PLACE[q]], at_t(d))
    for h in range(2):
        for q in (0, 1, 3, 2):
            go(tail_hbm.at[owner_rows(2, q), pl.ds(h * lane, lane)], relay.at[h, PLACE[q]],
               r_s.at[h, PLACE[q]], r_r.at[h, PLACE[q]], at_t(1 + 2 * (PLACE[q] % 2)))

    arrived(wall.at[2 * p1 + k], wb_s.at[0], wb_r.at[0])
    strip_to_core(2, p1)
    arrived(wall.at[2 * p12 + k], wb_s.at[1], wb_r.at[1])
    strip_to_core(3, p12)

    for i, other in enumerate((x, p1, p2, p12)):
        arrived(wall.at[2 * other + 1 - k], wc_s.at[i], wc_r.at[i])

    blocks = window // share
    for i in range(blocks):
        inv[pl.ds(i * share, share), pl.ds(i * share, share)] = wall[i, :, pl.ds(i * share, share)]
    size = share
    while size < window:
        count = size // share
        strip = min(size, 256)
        for base in range(0, window, 2 * size):
            top, low_rows = pl.ds(base, size), pl.ds(base + size, size)

            def below(i, _, base=base, size=size, count=count, strip=strip, top=top, low_rows=low_rows):
                start = pl.multiple_of(i * strip, strip)
                left = inv[pl.ds(base + size + start, strip), low_rows]
                under = wall[pl.ds(base // share + count, count), :, top].reshape(size, size)
                times = dot if size == share else dot_split
                tmp[pl.ds(0, strip), pl.ds(0, size)] = times(left, under)
                inv[pl.ds(base + size + start, strip), top] = -times(tmp[pl.ds(0, strip), pl.ds(0, size)], inv[top, top])
                return 0

            if strip == size:
                below(0, 0)
            else:
                lax.fori_loop(0, size // strip, below, 0)
        size *= 2

    def split_inverse(i, _):
        high, rest = halves(inv[rows_of(i), :])
        inv_hi[rows_of(i), :] = high
        inv_lo[rows_of(i), :] = rest
        return 0

    lax.fori_loop(0, window // 128, split_inverse, 0)

    def pass_tail(h):
        for q in range(SIDE):
            arrived(relay.at[h, q], r_s.at[h, q], r_r.at[h, q])
            go(relay.at[h, q], tbuf.at[2, q, pl.ds(0, depth), pl.ds(h * lane, lane)],
               f_s.at[h, q], f_r.at[h, q], at_t(1 + 2 * (q % 2)))

    def turn_panel(q, _):
        def split_rows(i, _):
            high, rest = halves(pbuf[q, rows_of(i), :])
            phi[rows_of(i), :] = high
            plo[rows_of(i), :] = rest
            return 0

        for i in range(pad // 128):
            split_rows(i, 0)
        place = pl.ds(pl.multiple_of(q * pad, pad), pad)
        for n in range(0, window, 256):
            deep, cols = pl.ds(n, window - n), pl.ds(n, 256)
            product = (
                mm(phi[:, deep], inv_hi[deep, cols])
                + mm(phi[:, deep], inv_lo[deep, cols])
                + mm(plo[:, deep], inv_hi[deep, cols])
            )
            high, rest = halves(-product.T)
            pthi[cols, place] = high
            ptlo[cols, place] = rest
        return 0

    def panel_here(q):
        for i in range(PARTS):
            if q != came_from(i):
                arrived(pbuf.at[q, part_rows(i)], p_s.at[0, i], p_r.at[q, i])

    locals_[1].wait()
    panel_here(1)
    panel_here(2)
    for q in range(3):
        turn_panel(q, 0)

    def take_tail(j, places, cols):
        for q in places:
            high, rest = halves(tbuf[j, q, :, cols])
            thi[pl.ds(q * pad, pad), cols] = high
            tlo[pl.ds(q * pad, pad), cols] = rest

    strip = 512

    def product(j, places, cols, fresh):
        take_tail(j, places, cols)
        deep = pl.ds(places[0] * pad, len(places) * pad)

        def one(i, _):
            rows = rows_of(i, strip)
            total = (
                mm(pthi[rows, deep], thi[deep, cols])
                + mm(pthi[rows, deep], tlo[deep, cols])
                + mm(ptlo[rows, deep], thi[deep, cols])
            )
            for h in range(total.shape[1] // lane):
                u = 2 * j + h + cols.start // lane
                piece = total[:, h * lane:(h + 1) * lane]
                sums[u, rows, :] = piece if fresh else sums[u, rows, :] + piece
            return 0

        for i in range(window // strip):
            one(i, 0)

    whole = pl.ds(0, width)
    def beside(j, places, fresh):
        for q in places:
            arrived(tbuf.at[j, q, pl.ds(0, depth)], t_s.at[1, q], t_r.at[j, q])
        product(j, places, whole, fresh)

    def cross(h, places, fresh):
        for q in places:
            arrived(tbuf.at[2, q, pl.ds(0, depth), pl.ds(h * lane, lane)], f_s.at[h, q], f_r.at[h, q])
        product(2, places, pl.ds(h * lane, lane), fresh)

    def lines(u, xx):
        return rows_of(xx, 2 * share) if u > 1 else rows_of(2 * xx + k, share)

    def height(u):
        return pl.ds(0, 2 * share if u > 1 else share)

    def to_core(u):
        for i in range(SIDE):
            go(sums.at[u, rows_of(2 * i + 1 - k, share)], core_in.at[u, i], c_s.at[u, i], c_r.at[u, i], partner)

    def to_first(u):
        if u < 2:
            for i in range(SIDE):
                arrived(core_in.at[u, i], c_s.at[u, i], c_r.at[u, i])
                rows = rows_of(2 * i + k, share)
                sums[u, rows, :] = sums[u, rows, :] + core_in[u, i]
        for i, other in ((1, p12), (0, p1)):
            go(sums.at[u, lines(u, other)], first_in.at[u, i, height(u)], a_s.at[u, i], a_r.at[u, i], at_x(p1))

    def to_second(u):
        for i, other in ((1, p2), (0, x)):
            arrived(first_in.at[u, i, height(u)], a_s.at[u, i], a_r.at[u, i])
            rows = lines(u, other)
            sums[u, rows, :] = sums[u, rows, :] + first_in[u, i, height(u), :]
            if i == 1:
                go(sums.at[u, rows], second_in.at[u, height(u)], b_s.at[u], b_r.at[u], at_x(p2))

    def to_last(u):
        j, h = u // 2, u % 2
        arrived(second_in.at[u, height(u)], b_s.at[u], b_r.at[u])
        rows = lines(u, x)
        sums[u, rows, :] = sums[u, rows, :] + second_in[u, height(u), :]
        if j:
            for i, core in enumerate((k, 1 - k)):
                go(sums.at[u, rows_of(2 * x + core, share)], last_in.at[k, SIDE - j, h],
                   l_s.at[i, u], l_r.at[k, SIDE - j, h], {"row": 2 * x + core, "col": place_at(j, 0)})

    def both(stage, j):
        stage(2 * j)
        stage(2 * j + 1)

    for copy in locals_[2:]:
        copy.wait()
    product(0, (0, 1, 2), whole, True)
    rhs_hi, rhs_lo = halves(rhs[...])
    own_hi, own_lo = inv_hi[rows_of(r, share), :], inv_lo[rows_of(r, share), :]
    own = mm_t(own_hi, rhs_hi) + mm_t(own_hi, rhs_lo) + mm_t(own_lo, rhs_hi)
    for h in range(2):
        sums[h] = sums[h] + own[:, h * lane:(h + 1) * lane]
    panel_here(3)
    turn_panel(3, 0)
    product(0, (3,), whole, False)
    both(to_core, 0)
    beside(1, (0,), True)
    both(to_first, 0)
    beside(1, (1, 2, 3), False)
    both(to_first, 1)
    beside(3, (0, 1, 2, 3), True)
    both(to_first, 3)
    both(to_second, 0)
    pass_tail(0)
    pass_tail(1)
    both(to_last, 0)
    both(to_second, 1)
    cross(0, (0, 1), True)
    cross(0, (2, 3), False)
    to_first(4)
    both(to_second, 3)
    both(to_last, 1)
    cross(1, (0, 1), True)
    cross(1, (2, 3), False)
    to_first(5)
    to_second(4)
    both(to_last, 3)
    to_second(5)
    to_last(4)
    to_last(5)

    rows = rows_of(r, share)
    for h in range(2):
        total = sums[h, rows, :]
        for core, d in ((k, 1), (1 - k, 1), (k, 3), (1 - k, 3), (k, 2), (1 - k, 2)):
            arrived(last_in.at[core, d, h], l_s.at[0, 0], l_r.at[core, d, h])
            total = total + last_in[core, d, h]
        out_ref[:, h * lane:(h + 1) * lane] = total

    for copy in pending:
        copy.wait_send()


def per_device(tail_vectors, lower_panel, window_rhs, window_block):
    columns = tail_vectors.shape[1]
    depth, window = lower_panel.shape
    share = window_rhs.shape[0]
    lane = columns // 2
    pad = -(-depth // 128) * 128
    groups = window // share
    dma = pltpu.SemaphoreType.DMA
    anywhere = pl.BlockSpec(memory_space=pl.ANY)
    return pl.pallas_call(
        kernel,
        out_shape=pltpu.VMEM((share, columns), F32),
        in_specs=[anywhere] * 4,
        out_specs=pl.BlockSpec(memory_space=pltpu.VMEM),
        scratch_shapes=[
            pltpu.VMEM((SIDE, SIDE, pad, columns), F32),
            pltpu.VMEM((2, SIDE, depth, lane), F32),
            pltpu.VMEM((SIDE, pad, window), F32),
            pltpu.VMEM((pad, window), BF16),
            pltpu.VMEM((pad, window), BF16),
            pltpu.VMEM((window, SIDE * pad), BF16),
            pltpu.VMEM((window, SIDE * pad), BF16),
            pltpu.VMEM((groups, share, window), F32),
            pltpu.VMEM((window, window), F32),
            pltpu.VMEM((window, window), BF16),
            pltpu.VMEM((window, window), BF16),
            pltpu.VMEM((256, window // 2), F32),
            pltpu.VMEM((share, columns), F32),
            pltpu.VMEM((SIDE * pad, columns), BF16),
            pltpu.VMEM((SIDE * pad, columns), BF16),
            pltpu.VMEM((2 * SIDE, window, lane), F32),
            pltpu.VMEM((2, SIDE, share, lane), F32),
            pltpu.VMEM((2 * SIDE, 2, 2 * share, lane), F32),
            pltpu.VMEM((2 * SIDE, 2 * share, lane), F32),
            pltpu.VMEM((2, SIDE, 2, share, lane), F32),
            dma((7,)),
            dma((SIDE,)), dma((SIDE,)), dma((3, SIDE)), dma((3, SIDE)),
            dma, dma, dma((2,)), dma((2,)), dma((SIDE,)), dma((SIDE,)),
            dma((3, PARTS)), dma((SIDE, PARTS)),
            dma((SIDE, SIDE)), dma((SIDE, SIDE)),
            dma((2, SIDE)), dma((2, SIDE)), dma((2, SIDE)), dma((2, SIDE)),
            dma((2, SIDE)), dma((2, SIDE)),
            dma((2 * SIDE, 2)), dma((2 * SIDE, 2)),
            dma((2 * SIDE,)), dma((2 * SIDE,)),
            dma((2, 2 * SIDE)), dma((2, SIDE, 2)),
        ],
        compiler_params=pltpu.CompilerParams(
            collective_id=0, has_side_effects=True, vmem_limit_bytes=65000 * 1024
        ),
    )(tail_vectors, lower_panel, window_block, window_rhs)


def solution(mesh):
    in_specs = (P("row", "col"), P(("row", "col"), None), P("row", "col"), P(("row", "col"), None))
    out_specs = P("row", "col")
    return jax.shard_map(per_device, mesh=mesh, in_specs=in_specs, out_specs=out_specs, check_vma=False)
```

```python
import functools

import jax
import jax.numpy as jnp
from jax import lax
from jax.experimental import pallas as pl
from jax.experimental.pallas import tpu as pltpu
from jax.sharding import PartitionSpec as P

MESH = pl.DeviceIdType.MESH
HIGHEST = lax.Precision.HIGHEST
F32 = jnp.float32
BF16 = jnp.bfloat16
SIDE = 4
PLACE = (0, 1, 3, 2)
CUTS = (13, 8, 7, 5, 10, 10, 10)
PARTS = len(CUTS)
FORTH = 4


def dot(a, b):
    return jnp.dot(a, b, precision=HIGHEST, preferred_element_type=F32)


def mm_t(a, b):
    return lax.dot_general(a, b, (((0,), (0,)), ((), ())), preferred_element_type=F32)


def mm(a, b):
    return jnp.dot(a, b, preferred_element_type=F32)


def halves(a):
    high = a.astype(BF16)
    return high, (a - high.astype(F32)).astype(BF16)


def dot_split(a, b):
    a_hi, a_lo = halves(a)
    b_hi, b_lo = halves(b)
    return mm(a_hi, b_hi) + mm(a_hi, b_lo) + mm(a_lo, b_hi)


def lower_inverse(block, base=32):
    size = block.shape[0]
    rows = lax.broadcasted_iota(jnp.int32, (size, size), 0)
    cols = lax.broadcasted_iota(jnp.int32, (size, size), 1)
    eye = jnp.where(rows == cols, 1.0, 0.0)
    diag_col = jnp.sum(jnp.where(rows == cols, block, 0.0), axis=1, keepdims=True)
    diag_row = jnp.sum(jnp.where(rows == cols, block, 0.0), axis=0, keepdims=True)
    near = (rows // base == cols // base) & (rows > cols)
    power = jnp.where(near, -block / diag_col, 0.0)
    inverse = eye + power
    reach = 2
    while reach < base:
        power = dot(power, power)
        inverse = inverse + dot(inverse, power)
        reach *= 2
    inverse = inverse / diag_row
    while base < size:
        below = (rows // (2 * base) == cols // (2 * base)) & (rows // base > cols // base)
        inverse = inverse - dot(dot(inverse, jnp.where(below, block, 0.0)), inverse)
        base *= 2
    return inverse


def kernel(
    tail_hbm, panel_hbm, block_hbm, rhs_hbm, out_ref,
    tbuf, relay, pbuf, phi, plo, pthi, ptlo, wall, inv, inv_hi, inv_lo, tmp, rhs, thi, tlo,
    sums, core_in, first_in, second_in, last_in,
    local_sem, wz_s, wz_r, wy_s, wy_r, wa_s, wa_r, wb_s, wb_r, wc_s, wc_r,
    p_s, p_r, t_s, t_r, r_s, r_r, f_s, f_r,
    c_s, c_r, a_s, a_r, b_s, b_r, l_s, l_r,
):
    depth, window = panel_hbm.shape
    thin = block_hbm.shape[0]
    share, width = rhs_hbm.shape
    lane = width // 2
    pad = pbuf.shape[1]
    unit = depth // sum(CUTS)
    r = lax.axis_index("row")
    c = lax.axis_index("col")
    x, k = r // 2, r % 2
    z, y = c // SIDE, c % SIDE
    low, mirror = x + 1 - 2 * (x % 2), SIDE - 1 - x
    p1 = k * mirror + (1 - k) * low
    p2 = k * low + (1 - k) * mirror
    p12 = (x + 2) % SIDE

    def place_at(dt, dp):
        zz = (z + dt * (1 - k) + dp * k + 2 * SIDE) % SIDE
        yy = (y + dt * k + dp * (1 - k) + 2 * SIDE) % SIDE
        return zz * SIDE + yy

    def at_t(d):
        return {"row": r, "col": place_at(d, 0)}

    def at_p(d):
        return {"row": r, "col": place_at(0, d)}

    def at_x(other):
        return {"row": 2 * other + k, "col": c}

    partner = {"row": 2 * x + 1 - k, "col": c}
    pending = []

    def remote(src, dst, send, recv, where):
        return pltpu.make_async_remote_copy(
            src_ref=src, dst_ref=dst, send_sem=send, recv_sem=recv, device_id=where, device_id_type=MESH
        )

    def go(src, dst, send, recv, where, keep=True):
        copy = remote(src, dst, send, recv, where)
        copy.start()
        if keep:
            pending.append(copy)
        return copy

    def arrived(dst, send, recv):
        remote(dst, dst, send, recv, partner).wait_recv()

    def owner_rows(dt, dp):
        return pl.ds(pl.multiple_of(place_at(dt, dp) * depth, 8), depth)

    def rows_of(index, size=128):
        return pl.ds(pl.multiple_of(index * size, size), size)

    own_thin = wall.at[r, pl.ds(pl.multiple_of(c * thin, 8), thin)]
    locals_ = [
        pltpu.make_async_copy(block_hbm, own_thin, local_sem.at[0]),
        pltpu.make_async_copy(panel_hbm, pbuf.at[0, pl.ds(0, depth)], local_sem.at[1]),
        pltpu.make_async_copy(rhs_hbm, rhs, local_sem.at[2]),
    ] + [
        pltpu.make_async_copy(tail_hbm.at[owner_rows(0, d)], tbuf.at[0, PLACE[d], pl.ds(0, depth)], local_sem.at[3 + d])
        for d in range(SIDE)
    ]
    for copy in locals_:
        copy.start()

    barrier = pltpu.get_barrier_semaphore()
    greeted = [at_x(p1), at_x(p2), partner] + [
        {"row": 2 * x + core, "col": place_at(*offset)}
        for core in range(2) for d in (1, 2, 3) for offset in ((d, 0), (0, d))
    ]
    for where in greeted:
        pl.semaphore_signal(barrier, inc=1, device_id=where, device_id_type=MESH)
    pl.semaphore_wait(barrier, len(greeted))

    def part_rows(i):
        return pl.ds(sum(CUTS[:i]) * unit, CUTS[i] * unit)

    def send_panel(i):
        go(panel_hbm.at[part_rows(i)], pbuf.at[2, part_rows(i)], p_s.at[0, i], p_r.at[2, i], at_p(1))
        go(panel_hbm.at[part_rows(i)], pbuf.at[1, part_rows(i)], p_s.at[1, i], p_r.at[1, i], at_p(3))

    for d in (2, 1, 3):
        go(block_hbm, own_thin, wz_s.at[d], wz_r.at[SIDE - d], at_t(d))
    send_panel(0)

    def clear(i, _):
        inv[rows_of(i), :] = jnp.zeros((128, window), F32)
        return 0

    lax.fori_loop(0, window // 128, clear, 0)
    zeros = jnp.zeros((pad - depth, width), F32)
    for j in range(SIDE):
        for q in range(SIDE):
            tbuf[j, q, pl.ds(depth, pad - depth), :] = zeros
    for q in range(SIDE):
        pbuf[q, pl.ds(depth, pad - depth), :] = jnp.zeros((pad - depth, window), F32)

    def thin_rows(dt, dp):
        return wall.at[r, pl.ds(pl.multiple_of(place_at(dt, dp) * thin, 8), thin)]

    locals_[0].wait()
    for d in (1, 3, 2):
        arrived(thin_rows(d, 0), wz_s.at[d], wz_r.at[d])
    thin_copies = []
    pc = k * z + (1 - k) * y
    near = 1 - 2 * (pc % 2)

    def swap_thin(sem, mine, where):
        for d in range(SIDE):
            side = 1 if d < 2 else -1
            rows = thin_rows(d, side * mine)
            thin_copies.append(go(rows, rows, wy_s.at[sem, d], wy_r.at[sem, d], at_p(side * where), False))

    def thin_here(sem, theirs):
        for d in range(SIDE):
            arrived(thin_rows(d, theirs if d < 2 else -theirs), wy_s.at[sem, d], wy_r.at[sem, d])

    swap_thin(0, 0, near)
    send_panel(1)
    thin_here(0, near)
    swap_thin(1, 0, -near)
    swap_thin(2, near, -near)
    for i in range(2, PARTS):
        send_panel(i)
    thin_here(1, -near)
    thin_here(2, 2)
    for copy in thin_copies:
        copy.wait_send()

    diag = rows_of(r, share)
    wall[r, :, diag] = lower_inverse(wall[r, :, diag])
    def came_from(i):
        return 2 if i < FORTH else 1

    def pass_panel(i):
        side = came_from(i)
        arrived(pbuf.at[side, part_rows(i)], p_s.at[2, i], p_r.at[side, i])
        go(pbuf.at[side, part_rows(i)], pbuf.at[3, part_rows(i)], p_s.at[2, i], p_r.at[3, i], at_p(2 * side - 3))

    def strip_to_core(i, other):
        go(wall.at[2 * other + k], wall.at[2 * other + k], wc_s.at[i], wc_r.at[i], partner)

    go(wall.at[r], wall.at[r], wa_s, wa_r, at_x(p2))
    go(wall.at[r], wall.at[r], wb_s.at[0], wb_r.at[0], at_x(p1))
    strip_to_core(0, x)
    for i in range(PARTS - 1):
        pass_panel(i)
    arrived(wall.at[2 * p2 + k], wa_s, wa_r)
    go(wall.at[2 * p2 + k], wall.at[2 * p2 + k], wb_s.at[1], wb_r.at[1], at_x(p1))
    strip_to_core(1, p2)
    pass_panel(PARTS - 1)

    for q in (0, 1, 3, 2):
        for d in (1, 3):
            go(tail_hbm.at[owner_rows(d, q)], tbuf.at[SIDE - d, PLACE[q], pl.ds(0, depth)],
               t_s.at[d, PLACE[q]], t_r.at[SIDE - d, PLACE[q]], at_t(d))
    for h in range(2):
        for q in (0, 1, 3, 2):
            go(tail_hbm.at[owner_rows(2, q), pl.ds(h * lane, lane)], relay.at[h, PLACE[q]],
               r_s.at[h, PLACE[q]], r_r.at[h, PLACE[q]], at_t(1 + 2 * (PLACE[q] % 2)))

    arrived(wall.at[2 * p1 + k], wb_s.at[0], wb_r.at[0])
    strip_to_core(2, p1)
    arrived(wall.at[2 * p12 + k], wb_s.at[1], wb_r.at[1])
    strip_to_core(3, p12)

    for i, other in enumerate((x, p1, p2, p12)):
        arrived(wall.at[2 * other + 1 - k], wc_s.at[i], wc_r.at[i])

    blocks = window // share
    for i in range(blocks):
        inv[pl.ds(i * share, share), pl.ds(i * share, share)] = wall[i, :, pl.ds(i * share, share)]
    size = share
    while size < window:
        count = size // share
        strip = min(size, 256)
        for base in range(0, window, 2 * size):
            top, low_rows = pl.ds(base, size), pl.ds(base + size, size)

            def below(i, _, base=base, size=size, count=count, strip=strip, top=top, low_rows=low_rows):
                start = i * strip
                left = inv[pl.ds(base + size + start, strip), low_rows]
                under = wall[pl.ds(base // share + count, count), :, top].reshape(size, size)
                times = dot if size == share else dot_split
                tmp[pl.ds(0, strip), pl.ds(0, size)] = times(left, under)
                inv[pl.ds(base + size + start, strip), top] = -times(tmp[pl.ds(0, strip), pl.ds(0, size)], inv[top, top])
                return 0

            for i in range(size // strip):
                below(i, 0)
        size *= 2

    def split_inverse(i, _):
        high, rest = halves(inv[rows_of(i), :])
        inv_hi[rows_of(i), :] = high
        inv_lo[rows_of(i), :] = rest
        return 0

    for i in range(window // 128):
        split_inverse(i, 0)

    def pass_tail(h):
        for q in range(SIDE):
            arrived(relay.at[h, q], r_s.at[h, q], r_r.at[h, q])
            go(relay.at[h, q], tbuf.at[2, q, pl.ds(0, depth), pl.ds(h * lane, lane)],
               f_s.at[h, q], f_r.at[h, q], at_t(1 + 2 * (q % 2)))

    def turn_panel(q, _):
        def split_rows(i, _):
            high, rest = halves(pbuf[q, rows_of(i), :])
            phi[rows_of(i), :] = high
            plo[rows_of(i), :] = rest
            return 0

        for i in range(pad // 128):
            split_rows(i, 0)
        place = pl.ds(pl.multiple_of(q * pad, pad), pad)
        for n in range(0, window, 256):
            deep, cols = pl.ds(n, window - n), pl.ds(n, 256)
            product = (
                mm(phi[:, deep], inv_hi[deep, cols])
                + mm(phi[:, deep], inv_lo[deep, cols])
                + mm(plo[:, deep], inv_hi[deep, cols])
            )
            high, rest = halves(-product.T)
            pthi[cols, place] = high
            ptlo[cols, place] = rest
        return 0

    def panel_here(q):
        for i in range(PARTS):
            if q != came_from(i):
                arrived(pbuf.at[q, part_rows(i)], p_s.at[0, i], p_r.at[q, i])

    locals_[1].wait()
    panel_here(1)
    panel_here(2)
    for q in range(3):
        turn_panel(q, 0)

    def take_tail(j, places, cols):
        for q in places:
            high, rest = halves(tbuf[j, q, :, cols])
            thi[pl.ds(q * pad, pad), cols] = high
            tlo[pl.ds(q * pad, pad), cols] = rest

    strip = 512

    def product(j, places, cols, fresh):
        take_tail(j, places, cols)
        deep = pl.ds(places[0] * pad, len(places) * pad)

        def one(i, _):
            rows = rows_of(i, strip)
            total = (
                mm(pthi[rows, deep], thi[deep, cols])
                + mm(pthi[rows, deep], tlo[deep, cols])
                + mm(ptlo[rows, deep], thi[deep, cols])
            )
            for h in range(total.shape[1] // lane):
                u = 2 * j + h + cols.start // lane
                piece = total[:, h * lane:(h + 1) * lane]
                sums[u, rows, :] = piece if fresh else sums[u, rows, :] + piece
            return 0

        for i in range(window // strip):
            one(i, 0)

    whole = pl.ds(0, width)
    def beside(j, places, fresh):
        for q in places:
            arrived(tbuf.at[j, q, pl.ds(0, depth)], t_s.at[1, q], t_r.at[j, q])
        product(j, places, whole, fresh)

    def cross(h, places, fresh):
        for q in places:
            arrived(tbuf.at[2, q, pl.ds(0, depth), pl.ds(h * lane, lane)], f_s.at[h, q], f_r.at[h, q])
        product(2, places, pl.ds(h * lane, lane), fresh)

    def cores(u):
        return range(2 if u > 1 else 1)

    def line(u, xx, e):
        return rows_of(2 * xx + (e if u > 1 else k), share)

    def piece(e):
        return pl.ds(e * share, share)

    def to_core(u):
        for i in range(SIDE):
            go(sums.at[u, rows_of(2 * i + 1 - k, share)], core_in.at[u, i], c_s.at[u, i], c_r.at[u, i], partner)

    def to_first(u):
        if u < 2:
            for i in range(SIDE):
                arrived(core_in.at[u, i], c_s.at[u, i], c_r.at[u, i])
                rows = rows_of(2 * i + k, share)
                sums[u, rows, :] = sums[u, rows, :] + core_in[u, i]
        for i, other in ((1, p12), (0, p1)):
            for e in cores(u):
                go(sums.at[u, line(u, other, e)], first_in.at[u, i, piece(e)],
                   a_s.at[u, i, e], a_r.at[u, i, e], at_x(p1))

    def to_second(u):
        for i, other in ((1, p2), (0, x)):
            for e in cores(u):
                arrived(first_in.at[u, i, piece(e)], a_s.at[u, i, e], a_r.at[u, i, e])
                rows = line(u, other, e)
                sums[u, rows, :] = sums[u, rows, :] + first_in[u, i, piece(e), :]
                if i == 1:
                    go(sums.at[u, rows], second_in.at[u, piece(e)], b_s.at[u, e], b_r.at[u, e], at_x(p2))

    def to_last(u):
        j, h = u // 2, u % 2
        for e in cores(u):
            arrived(second_in.at[u, piece(e)], b_s.at[u, e], b_r.at[u, e])
            rows = line(u, x, e)
            sums[u, rows, :] = sums[u, rows, :] + second_in[u, piece(e), :]
            if j:
                go(sums.at[u, rows], last_in.at[k, SIDE - j, h], l_s.at[e, u], l_r.at[k, SIDE - j, h],
                   {"row": 2 * x + e, "col": place_at(j, 0)})

    def both(stage, j):
        stage(2 * j)
        stage(2 * j + 1)

    for copy in locals_[2:]:
        copy.wait()
    product(0, (0, 1, 2), whole, True)
    rhs_hi, rhs_lo = halves(rhs[...])
    own_hi, own_lo = inv_hi[rows_of(r, share), :], inv_lo[rows_of(r, share), :]
    own = mm_t(own_hi, rhs_hi) + mm_t(own_hi, rhs_lo) + mm_t(own_lo, rhs_hi)
    for h in range(2):
        sums[h] = sums[h] + own[:, h * lane:(h + 1) * lane]
    panel_here(3)
    turn_panel(3, 0)
    product(0, (3,), whole, False)
    both(to_core, 0)
    beside(1, (0,), True)
    both(to_first, 0)
    beside(1, (1, 2, 3), False)
    both(to_first, 1)
    beside(3, (0, 1, 2, 3), True)
    both(to_first, 3)
    both(to_second, 0)
    pass_tail(0)
    pass_tail(1)
    both(to_last, 0)
    both(to_second, 1)
    cross(0, (0, 1), True)
    cross(0, (2, 3), False)
    to_first(4)
    both(to_second, 3)
    both(to_last, 1)
    cross(1, (0, 1), True)
    cross(1, (2, 3), False)
    to_first(5)
    to_second(4)
    both(to_last, 3)
    to_second(5)
    to_last(4)
    to_last(5)

    rows = rows_of(r, share)
    for h in range(2):
        total = sums[h, rows, :]
        for core, d in ((k, 1), (1 - k, 1), (k, 3), (1 - k, 3), (k, 2), (1 - k, 2)):
            arrived(last_in.at[core, d, h], l_s.at[0, 0], l_r.at[core, d, h])
            total = total + last_in[core, d, h]
        out_ref[:, h * lane:(h + 1) * lane] = total

    for copy in pending:
        copy.wait_send()


def per_device(tail_vectors, lower_panel, window_rhs, window_block):
    columns = tail_vectors.shape[1]
    depth, window = lower_panel.shape
    share = window_rhs.shape[0]
    lane = columns // 2
    pad = -(-depth // 128) * 128
    groups = window // share
    dma = pltpu.SemaphoreType.DMA
    anywhere = pl.BlockSpec(memory_space=pl.ANY)
    return pl.pallas_call(
        kernel,
        out_shape=pltpu.VMEM((share, columns), F32),
        in_specs=[anywhere] * 4,
        out_specs=pl.BlockSpec(memory_space=pltpu.VMEM),
        scratch_shapes=[
            pltpu.VMEM((SIDE, SIDE, pad, columns), F32),
            pltpu.VMEM((2, SIDE, depth, lane), F32),
            pltpu.VMEM((SIDE, pad, window), F32),
            pltpu.VMEM((pad, window), BF16),
            pltpu.VMEM((pad, window), BF16),
            pltpu.VMEM((window, SIDE * pad), BF16),
            pltpu.VMEM((window, SIDE * pad), BF16),
            pltpu.VMEM((groups, share, window), F32),
            pltpu.VMEM((window, window), F32),
            pltpu.VMEM((window, window), BF16),
            pltpu.VMEM((window, window), BF16),
            pltpu.VMEM((256, window // 2), F32),
            pltpu.VMEM((share, columns), F32),
            pltpu.VMEM((SIDE * pad, columns), BF16),
            pltpu.VMEM((SIDE * pad, columns), BF16),
            pltpu.VMEM((2 * SIDE, window, lane), F32),
            pltpu.VMEM((2, SIDE, share, lane), F32),
            pltpu.VMEM((2 * SIDE, 2, 2 * share, lane), F32),
            pltpu.VMEM((2 * SIDE, 2 * share, lane), F32),
            pltpu.VMEM((2, SIDE, 2, share, lane), F32),
            dma((7,)),
            dma((SIDE,)), dma((SIDE,)), dma((3, SIDE)), dma((3, SIDE)),
            dma, dma, dma((2,)), dma((2,)), dma((SIDE,)), dma((SIDE,)),
            dma((3, PARTS)), dma((SIDE, PARTS)),
            dma((SIDE, SIDE)), dma((SIDE, SIDE)),
            dma((2, SIDE)), dma((2, SIDE)), dma((2, SIDE)), dma((2, SIDE)),
            dma((2, SIDE)), dma((2, SIDE)),
            dma((2 * SIDE, 2, 2)), dma((2 * SIDE, 2, 2)),
            dma((2 * SIDE, 2)), dma((2 * SIDE, 2)),
            dma((2, 2 * SIDE)), dma((2, SIDE, 2)),
        ],
        compiler_params=pltpu.CompilerParams(
            collective_id=0, has_side_effects=True, vmem_limit_bytes=65000 * 1024
        ),
    )(tail_vectors, lower_panel, window_block, window_rhs)


def solution(mesh):
    in_specs = (P("row", "col"), P(("row", "col"), None), P("row", "col"), P(("row", "col"), None))
    out_specs = P("row", "col")
    return jax.shard_map(per_device, mesh=mesh, in_specs=in_specs, out_specs=out_specs, check_vma=False)
```

```python
import functools

import jax
import jax.numpy as jnp
from jax import lax
from jax.experimental import pallas as pl
from jax.experimental.pallas import tpu as pltpu
from jax.sharding import PartitionSpec as P

MESH = pl.DeviceIdType.MESH
HIGHEST = lax.Precision.HIGHEST
F32 = jnp.float32
BF16 = jnp.bfloat16
SIDE = 4
PLACE = (0, 1, 3, 2)
CUTS = (13, 8, 7, 5, 10, 10, 10)
PARTS = len(CUTS)
FORTH = 4


def dot(a, b):
    return jnp.dot(a, b, precision=HIGHEST, preferred_element_type=F32)


def mm_t(a, b):
    return lax.dot_general(a, b, (((0,), (0,)), ((), ())), preferred_element_type=F32)


def mm(a, b):
    return jnp.dot(a, b, preferred_element_type=F32)


def halves(a):
    high = a.astype(BF16)
    return high, (a - high.astype(F32)).astype(BF16)


def dot_split(a, b):
    a_hi, a_lo = halves(a)
    b_hi, b_lo = halves(b)
    return mm(a_hi, b_hi) + mm(a_hi, b_lo) + mm(a_lo, b_hi)


def lower_inverse(block, base=32):
    size = block.shape[0]
    rows = lax.broadcasted_iota(jnp.int32, (size, size), 0)
    cols = lax.broadcasted_iota(jnp.int32, (size, size), 1)
    eye = jnp.where(rows == cols, 1.0, 0.0)
    diag_col = jnp.sum(jnp.where(rows == cols, block, 0.0), axis=1, keepdims=True)
    diag_row = jnp.sum(jnp.where(rows == cols, block, 0.0), axis=0, keepdims=True)
    near = (rows // base == cols // base) & (rows > cols)
    power = jnp.where(near, -block / diag_col, 0.0)
    inverse = eye + power
    reach = 2
    while reach < base:
        power = dot(power, power)
        inverse = inverse + dot(inverse, power)
        reach *= 2
    inverse = inverse / diag_row
    while base < size:
        below = (rows // (2 * base) == cols // (2 * base)) & (rows // base > cols // base)
        inverse = inverse - dot(dot(inverse, jnp.where(below, block, 0.0)), inverse)
        base *= 2
    return inverse


def kernel(
    tail_hbm, panel_hbm, block_hbm, rhs_hbm, out_ref,
    tbuf, relay, pbuf, phi, plo, pthi, ptlo, wall, inv, inv_hi, inv_lo, tmp, rhs, thi, tlo,
    sums, core_in, first_in, second_in, last_in,
    local_sem, wz_s, wz_r, wy_s, wy_r, wa_s, wa_r, wb_s, wb_r, wc_s, wc_r,
    p_s, p_r, t_s, t_r, r_s, r_r, f_s, f_r,
    c_s, c_r, a_s, a_r, b_s, b_r, l_s, l_r,
):
    depth, window = panel_hbm.shape
    thin = block_hbm.shape[0]
    share, width = rhs_hbm.shape
    lane = width // 2
    pad = pbuf.shape[1]
    unit = depth // sum(CUTS)
    r = lax.axis_index("row")
    c = lax.axis_index("col")
    x, k = r // 2, r % 2
    z, y = c // SIDE, c % SIDE
    low, mirror = x + 1 - 2 * (x % 2), SIDE - 1 - x
    p1 = k * mirror + (1 - k) * low
    p2 = k * low + (1 - k) * mirror
    p12 = (x + 2) % SIDE

    def place_at(dt, dp):
        zz = (z + dt * (1 - k) + dp * k + 2 * SIDE) % SIDE
        yy = (y + dt * k + dp * (1 - k) + 2 * SIDE) % SIDE
        return zz * SIDE + yy

    def at_t(d):
        return {"row": r, "col": place_at(d, 0)}

    def at_p(d):
        return {"row": r, "col": place_at(0, d)}

    def at_x(other):
        return {"row": 2 * other + k, "col": c}

    partner = {"row": 2 * x + 1 - k, "col": c}
    pending = []

    def remote(src, dst, send, recv, where):
        return pltpu.make_async_remote_copy(
            src_ref=src, dst_ref=dst, send_sem=send, recv_sem=recv, device_id=where, device_id_type=MESH
        )

    def go(src, dst, send, recv, where, keep=True):
        copy = remote(src, dst, send, recv, where)
        copy.start()
        if keep:
            pending.append(copy)
        return copy

    def arrived(dst, send, recv):
        remote(dst, dst, send, recv, partner).wait_recv()

    def owner_rows(dt, dp):
        return pl.ds(pl.multiple_of(place_at(dt, dp) * depth, 8), depth)

    def rows_of(index, size=128):
        return pl.ds(pl.multiple_of(index * size, size), size)

    own_thin = wall.at[r, pl.ds(pl.multiple_of(c * thin, 8), thin)]
    locals_ = [
        pltpu.make_async_copy(block_hbm, own_thin, local_sem.at[0]),
        pltpu.make_async_copy(panel_hbm, pbuf.at[0, pl.ds(0, depth)], local_sem.at[1]),
        pltpu.make_async_copy(rhs_hbm, rhs, local_sem.at[2]),
    ] + [
        pltpu.make_async_copy(tail_hbm.at[owner_rows(0, d)], tbuf.at[0, PLACE[d], pl.ds(0, depth)], local_sem.at[3 + d])
        for d in range(SIDE)
    ]
    for copy in locals_:
        copy.start()

    barrier = pltpu.get_barrier_semaphore()
    greeted = [at_x(p1), at_x(p2), partner] + [
        {"row": 2 * x + core, "col": place_at(*offset)}
        for core in range(2) for d in (1, 2, 3) for offset in ((d, 0), (0, d))
    ]
    for where in greeted:
        pl.semaphore_signal(barrier, inc=1, device_id=where, device_id_type=MESH)
    pl.semaphore_wait(barrier, len(greeted))

    def part_rows(i):
        return pl.ds(sum(CUTS[:i]) * unit, CUTS[i] * unit)

    def send_panel(i):
        go(panel_hbm.at[part_rows(i)], pbuf.at[2, part_rows(i)], p_s.at[0, i], p_r.at[2, i], at_p(1))
        go(panel_hbm.at[part_rows(i)], pbuf.at[1, part_rows(i)], p_s.at[1, i], p_r.at[1, i], at_p(3))

    for d in (2, 1, 3):
        go(block_hbm, own_thin, wz_s.at[d], wz_r.at[SIDE - d], at_t(d))
    send_panel(0)

    def clear(i, _):
        inv[rows_of(i), :] = jnp.zeros((128, window), F32)
        return 0

    lax.fori_loop(0, window // 128, clear, 0)
    zeros = jnp.zeros((pad - depth, width), F32)
    for j in range(SIDE):
        for q in range(SIDE):
            tbuf[j, q, pl.ds(depth, pad - depth), :] = zeros
    for q in range(SIDE):
        pbuf[q, pl.ds(depth, pad - depth), :] = jnp.zeros((pad - depth, window), F32)

    def thin_rows(dt, dp):
        return wall.at[r, pl.ds(pl.multiple_of(place_at(dt, dp) * thin, 8), thin)]

    locals_[0].wait()
    for d in (1, 3, 2):
        arrived(thin_rows(d, 0), wz_s.at[d], wz_r.at[d])
    thin_copies = []
    pc = k * z + (1 - k) * y
    near = 1 - 2 * (pc % 2)

    def swap_thin(sem, mine, where):
        for d in range(SIDE):
            side = 1 if d < 2 else -1
            rows = thin_rows(d, side * mine)
            thin_copies.append(go(rows, rows, wy_s.at[sem, d], wy_r.at[sem, d], at_p(side * where), False))

    def thin_here(sem, theirs):
        for d in range(SIDE):
            arrived(thin_rows(d, theirs if d < 2 else -theirs), wy_s.at[sem, d], wy_r.at[sem, d])

    swap_thin(0, 0, near)
    send_panel(1)
    thin_here(0, near)
    swap_thin(1, 0, -near)
    swap_thin(2, near, -near)
    for i in range(2, PARTS):
        send_panel(i)
    thin_here(1, -near)
    thin_here(2, 2)
    for copy in thin_copies:
        copy.wait_send()

    diag = rows_of(r, share)
    wall[r, :, diag] = lower_inverse(wall[r, :, diag])
    def came_from(i):
        return 2 if i < FORTH else 1

    def pass_panel(i):
        side = came_from(i)
        arrived(pbuf.at[side, part_rows(i)], p_s.at[2, i], p_r.at[side, i])
        go(pbuf.at[side, part_rows(i)], pbuf.at[3, part_rows(i)], p_s.at[2, i], p_r.at[3, i], at_p(2 * side - 3))

    def strip_to_core(i, other):
        go(wall.at[2 * other + k], wall.at[2 * other + k], wc_s.at[i], wc_r.at[i], partner)

    go(wall.at[r], wall.at[r], wa_s, wa_r, at_x(p2))
    go(wall.at[r], wall.at[r], wb_s.at[0], wb_r.at[0], at_x(p1))
    strip_to_core(0, x)
    for i in range(PARTS - 1):
        pass_panel(i)
    arrived(wall.at[2 * p2 + k], wa_s, wa_r)
    go(wall.at[2 * p2 + k], wall.at[2 * p2 + k], wb_s.at[1], wb_r.at[1], at_x(p1))
    strip_to_core(1, p2)
    pass_panel(PARTS - 1)

    for q in (0, 1, 3, 2):
        for d in (1, 3):
            go(tail_hbm.at[owner_rows(d, q)], tbuf.at[SIDE - d, PLACE[q], pl.ds(0, depth)],
               t_s.at[d, PLACE[q]], t_r.at[SIDE - d, PLACE[q]], at_t(d))
    for h in range(2):
        for q in (0, 1, 3, 2):
            go(tail_hbm.at[owner_rows(2, q), pl.ds(h * lane, lane)], relay.at[h, PLACE[q]],
               r_s.at[h, PLACE[q]], r_r.at[h, PLACE[q]], at_t(1 + 2 * (PLACE[q] % 2)))

    arrived(wall.at[2 * p1 + k], wb_s.at[0], wb_r.at[0])
    strip_to_core(2, p1)
    arrived(wall.at[2 * p12 + k], wb_s.at[1], wb_r.at[1])
    strip_to_core(3, p12)

    for i, other in enumerate((x, p1, p2, p12)):
        arrived(wall.at[2 * other + 1 - k], wc_s.at[i], wc_r.at[i])

    blocks = window // share
    for i in range(blocks):
        inv[pl.ds(i * share, share), pl.ds(i * share, share)] = wall[i, :, pl.ds(i * share, share)]
    size = share
    while size < window:
        count = size // share
        strip = min(size, 256)
        for base in range(0, window, 2 * size):
            top, low_rows = pl.ds(base, size), pl.ds(base + size, size)

            def below(i, _, base=base, size=size, count=count, strip=strip, top=top, low_rows=low_rows):
                start = i * strip
                left = inv[pl.ds(base + size + start, strip), low_rows]
                under = wall[pl.ds(base // share + count, count), :, top].reshape(size, size)
                times = dot if size == share else dot_split
                tmp[pl.ds(0, strip), pl.ds(0, size)] = times(left, under)
                inv[pl.ds(base + size + start, strip), top] = -times(tmp[pl.ds(0, strip), pl.ds(0, size)], inv[top, top])
                return 0

            for i in range(size // strip):
                below(i, 0)
        size *= 2

    def split_inverse(i, _):
        high, rest = halves(inv[rows_of(i), :])
        inv_hi[rows_of(i), :] = high
        inv_lo[rows_of(i), :] = rest
        return 0

    for i in range(window // 128):
        split_inverse(i, 0)

    def pass_tail(h):
        for q in range(SIDE):
            arrived(relay.at[h, q], r_s.at[h, q], r_r.at[h, q])
            go(relay.at[h, q], tbuf.at[2, q, pl.ds(0, depth), pl.ds(h * lane, lane)],
               f_s.at[h, q], f_r.at[h, q], at_t(1 + 2 * (q % 2)))

    def turn_panel(q, _):
        def split_rows(i, _):
            high, rest = halves(pbuf[q, rows_of(i), :])
            phi[rows_of(i), :] = high
            plo[rows_of(i), :] = rest
            return 0

        for i in range(pad // 128):
            split_rows(i, 0)
        place = pl.ds(pl.multiple_of(q * pad, pad), pad)
        for n in range(0, window, 256):
            deep, cols = pl.ds(n, window - n), pl.ds(n, 256)
            product = (
                mm(phi[:, deep], inv_hi[deep, cols])
                + mm(phi[:, deep], inv_lo[deep, cols])
                + mm(plo[:, deep], inv_hi[deep, cols])
            )
            high, rest = halves(-product.T)
            pthi[cols, place] = high
            ptlo[cols, place] = rest
        return 0

    def panel_here(q):
        for i in range(PARTS):
            if q != came_from(i):
                arrived(pbuf.at[q, part_rows(i)], p_s.at[0, i], p_r.at[q, i])

    locals_[1].wait()
    panel_here(1)
    panel_here(2)
    for q in range(3):
        turn_panel(q, 0)

    def take_tail(j, places, cols):
        for q in places:
            high, rest = halves(tbuf[j, q, :, cols])
            thi[pl.ds(q * pad, pad), cols] = high
            tlo[pl.ds(q * pad, pad), cols] = rest

    strip = 512

    def product(j, places, cols, fresh):
        take_tail(j, places, cols)
        deep = pl.ds(places[0] * pad, len(places) * pad)

        def one(i, _):
            rows = rows_of(i, strip)
            total = (
                mm(pthi[rows, deep], thi[deep, cols])
                + mm(pthi[rows, deep], tlo[deep, cols])
                + mm(ptlo[rows, deep], thi[deep, cols])
            )
            for h in range(total.shape[1] // lane):
                u = 2 * j + h + cols.start // lane
                piece = total[:, h * lane:(h + 1) * lane]
                sums[u, rows, :] = piece if fresh else sums[u, rows, :] + piece
            return 0

        for i in range(window // strip):
            one(i, 0)

    whole = pl.ds(0, width)
    def beside(j, places, fresh):
        for q in places:
            arrived(tbuf.at[j, q, pl.ds(0, depth)], t_s.at[1, q], t_r.at[j, q])
        product(j, places, whole, fresh)

    def cross(h, places, fresh):
        for q in places:
            arrived(tbuf.at[2, q, pl.ds(0, depth), pl.ds(h * lane, lane)], f_s.at[h, q], f_r.at[h, q])
        product(2, places, pl.ds(h * lane, lane), fresh)

    def cores(u):
        return range(2 if u > 1 else 1)

    def line(u, xx, e):
        return rows_of(2 * xx + (e if u > 1 else k), share)

    def piece(e):
        return pl.ds(e * share, share)

    def to_core(u):
        for i in range(SIDE):
            go(sums.at[u, rows_of(2 * i + 1 - k, share)], core_in.at[u, i], c_s.at[u, i], c_r.at[u, i], partner)

    def to_first(u):
        if u < 2:
            for i in range(SIDE):
                arrived(core_in.at[u, i], c_s.at[u, i], c_r.at[u, i])
                rows = rows_of(2 * i + k, share)
                sums[u, rows, :] = sums[u, rows, :] + core_in[u, i]
        for i, other in ((1, p12), (0, p1)):
            for e in cores(u):
                go(sums.at[u, line(u, other, e)], first_in.at[u, i, piece(e)],
                   a_s.at[u, i, e], a_r.at[u, i, e], at_x(p1))

    def to_second(u):
        for i, other in ((1, p2), (0, x)):
            for e in cores(u):
                arrived(first_in.at[u, i, piece(e)], a_s.at[u, i, e], a_r.at[u, i, e])
                rows = line(u, other, e)
                sums[u, rows, :] = sums[u, rows, :] + first_in[u, i, piece(e), :]
                if i == 1:
                    go(sums.at[u, rows], second_in.at[u, piece(e)], b_s.at[u, e], b_r.at[u, e], at_x(p2))

    def to_last(u):
        j, h = u // 2, u % 2
        for e in cores(u):
            arrived(second_in.at[u, piece(e)], b_s.at[u, e], b_r.at[u, e])
            rows = line(u, x, e)
            sums[u, rows, :] = sums[u, rows, :] + second_in[u, piece(e), :]
            if j:
                go(sums.at[u, rows], last_in.at[k, SIDE - j, h], l_s.at[e, u], l_r.at[k, SIDE - j, h],
                   {"row": 2 * x + e, "col": place_at(j, 0)})

    def both(stage, j):
        stage(2 * j)
        stage(2 * j + 1)

    for copy in locals_[2:]:
        copy.wait()
    product(0, (0, 1, 2), whole, True)
    rhs_hi, rhs_lo = halves(rhs[...])
    own_hi, own_lo = inv_hi[rows_of(r, share), :], inv_lo[rows_of(r, share), :]
    own = mm_t(own_hi, rhs_hi) + mm_t(own_hi, rhs_lo) + mm_t(own_lo, rhs_hi)
    for h in range(2):
        sums[h] = sums[h] + own[:, h * lane:(h + 1) * lane]
    panel_here(3)
    turn_panel(3, 0)
    product(0, (3,), whole, False)
    both(to_core, 0)
    beside(1, (0,), True)
    both(to_first, 0)
    beside(1, (1, 2, 3), False)
    both(to_first, 1)
    beside(3, (0, 1, 2, 3), True)
    both(to_first, 3)
    both(to_second, 0)
    pass_tail(0)
    pass_tail(1)
    both(to_last, 0)
    both(to_second, 1)
    cross(0, (0, 1), True)
    cross(0, (2, 3), False)
    to_first(4)
    both(to_second, 3)
    both(to_last, 1)
    cross(1, (0, 1), True)
    cross(1, (2, 3), False)
    to_first(5)
    both(to_last, 3)
    to_second(5)
    to_second(4)
    to_last(5)
    to_last(4)

    rows = rows_of(r, share)
    for h in range(2):
        total = sums[h, rows, :]
        for core, d in ((k, 1), (1 - k, 1), (k, 3), (1 - k, 3), (k, 2), (1 - k, 2)):
            arrived(last_in.at[core, d, h], l_s.at[0, 0], l_r.at[core, d, h])
            total = total + last_in[core, d, h]
        out_ref[:, h * lane:(h + 1) * lane] = total

    for copy in pending:
        copy.wait_send()


def per_device(tail_vectors, lower_panel, window_rhs, window_block):
    columns = tail_vectors.shape[1]
    depth, window = lower_panel.shape
    share = window_rhs.shape[0]
    lane = columns // 2
    pad = -(-depth // 128) * 128
    groups = window // share
    dma = pltpu.SemaphoreType.DMA
    anywhere = pl.BlockSpec(memory_space=pl.ANY)
    return pl.pallas_call(
        kernel,
        out_shape=pltpu.VMEM((share, columns), F32),
        in_specs=[anywhere] * 4,
        out_specs=pl.BlockSpec(memory_space=pltpu.VMEM),
        scratch_shapes=[
            pltpu.VMEM((SIDE, SIDE, pad, columns), F32),
            pltpu.VMEM((2, SIDE, depth, lane), F32),
            pltpu.VMEM((SIDE, pad, window), F32),
            pltpu.VMEM((pad, window), BF16),
            pltpu.VMEM((pad, window), BF16),
            pltpu.VMEM((window, SIDE * pad), BF16),
            pltpu.VMEM((window, SIDE * pad), BF16),
            pltpu.VMEM((groups, share, window), F32),
            pltpu.VMEM((window, window), F32),
            pltpu.VMEM((window, window), BF16),
            pltpu.VMEM((window, window), BF16),
            pltpu.VMEM((256, window // 2), F32),
            pltpu.VMEM((share, columns), F32),
            pltpu.VMEM((SIDE * pad, columns), BF16),
            pltpu.VMEM((SIDE * pad, columns), BF16),
            pltpu.VMEM((2 * SIDE, window, lane), F32),
            pltpu.VMEM((2, SIDE, share, lane), F32),
            pltpu.VMEM((2 * SIDE, 2, 2 * share, lane), F32),
            pltpu.VMEM((2 * SIDE, 2 * share, lane), F32),
            pltpu.VMEM((2, SIDE, 2, share, lane), F32),
            dma((7,)),
            dma((SIDE,)), dma((SIDE,)), dma((3, SIDE)), dma((3, SIDE)),
            dma, dma, dma((2,)), dma((2,)), dma((SIDE,)), dma((SIDE,)),
            dma((3, PARTS)), dma((SIDE, PARTS)),
            dma((SIDE, SIDE)), dma((SIDE, SIDE)),
            dma((2, SIDE)), dma((2, SIDE)), dma((2, SIDE)), dma((2, SIDE)),
            dma((2, SIDE)), dma((2, SIDE)),
            dma((2 * SIDE, 2, 2)), dma((2 * SIDE, 2, 2)),
            dma((2 * SIDE, 2)), dma((2 * SIDE, 2)),
            dma((2, 2 * SIDE)), dma((2, SIDE, 2)),
        ],
        compiler_params=pltpu.CompilerParams(
            collective_id=0, has_side_effects=True, vmem_limit_bytes=65000 * 1024
        ),
    )(tail_vectors, lower_panel, window_block, window_rhs)


def solution(mesh):
    in_specs = (P("row", "col"), P(("row", "col"), None), P("row", "col"), P(("row", "col"), None))
    out_specs = P("row", "col")
    return jax.shard_map(per_device, mesh=mesh, in_specs=in_specs, out_specs=out_specs, check_vma=False)
```
